128 devices in a mesh: lat: 16 (over y, z), ch: 8 (over x, core).
Axes of the slice: x: 4, y: 4, z: 4, core: 2. Of those that a mesh axis runs over, the one named last changes fastest.
Arguments:
- field_in: bfloat16 [768, 384, 768], P('ch', 'lat'), may hold values from -80 to 80
- ln_gain: float32 [2, 768], P(None, 'ch'), may hold values from 0.5 to 1.5
- ln_shift: float32 [2, 768], P(None, 'ch'), may hold values from -1.5 to 1.5
- mix_first: bfloat16 [2, 2, 8, 96, 96], P(None, None, 'ch'), may hold values from -0.4375 to 0.4375
- mix_bias: bfloat16 [2, 2, 8, 96], P(None, None, 'ch'), may hold values from -3 to 3
- mix_second: bfloat16 [2, 2, 8, 96, 96], P(None, None, 'ch'), may hold values from -0.4375 to 0.4375
Outputs:
- field_out: bfloat16 [768, 384, 768], P('ch', 'lat')
The draws below stay inside these ranges and needn't reach their ends.
All inputs are finite; a program needn't handle non-finite values.
Results may differ from the reference program's by a relative error of at most 0.014.
Values may be sent and summed in bfloat16 or wider, within the bound.
A program may use at most 128 MiB of HBM per device.

```python
import math
import jax
import jax.numpy as jnp
from jax import lax

BLOCKS = 8
BLOCK = 96
CH = 768
LAT = 384
LON = 768
MODES = 384
LAYERS = 2


def draw_field_in(key, part):
    subkeys = jax.random.split(key, 4)
    base_draw = jnp.clip(jax.random.normal(subkeys[0], (CH, LAT, LON), jnp.float32), -5.0, 5.0)
    trend_rate = math.log(3.0)
    row_pos = jnp.arange(LAT, dtype=jnp.float32) / (LAT - 1)
    chan_pos = jnp.arange(CH, dtype=jnp.float32) / (CH - 1)
    row_scale = jnp.exp(trend_rate * (row_pos - 0.5) + jax.random.uniform(subkeys[1], (LAT,), jnp.float32, -0.6, 0.6))
    chan_scale = jnp.exp(trend_rate * (chan_pos - 0.5) + jax.random.uniform(subkeys[2], (CH,), jnp.float32, -0.6, 0.6))
    col_scale = jnp.exp(jax.random.uniform(subkeys[3], (LON,), jnp.float32, -0.4, 0.4))
    scaled = base_draw * chan_scale[:, None, None] * row_scale[None, :, None] * col_scale[None, None, :]
    return scaled.astype(jnp.bfloat16)


def level_of(key, shape, shards, least, top_value):
    level = 1.0
    for dim, blocks in shards:
        steps = jax.random.uniform(jax.random.fold_in(jax.random.fold_in(key, 6), dim), (blocks,), jnp.float32, least / len(shards), top_value / len(shards))
        level = level * jnp.repeat(jnp.exp(steps), shape[dim] // blocks).reshape((-1,) + (1,) * (len(shape) - 1 - dim))
    return level


def noise(stream_key, dims, scale, most, shards=(), held_as=jnp.bfloat16):
    entries = scale * jax.random.normal(stream_key, dims, jnp.float32)
    if shards:
        entries = entries * level_of(stream_key, dims, shards, -0.22, 0.18)
    return jnp.clip(entries, -most, most).astype(held_as)


def setup_inputs(seed: int = 0) -> dict:
    arg_keys = jax.random.split(jax.random.key(seed), 7)
    field_in = draw_field_in(jax.random.fold_in(arg_keys[6], 71), 0)
    ln_gain = jnp.clip(1.0 + 0.1 * jax.random.normal(arg_keys[1], (LAYERS, CH), jnp.float32), 0.5, 1.5)
    ln_shift = noise(arg_keys[2], (LAYERS, CH), 0.3, 1.5, ((1, 8),), jnp.float32)
    mix_first = noise(arg_keys[3], (LAYERS, 2, BLOCKS, BLOCK, BLOCK), (2 * BLOCK) ** -0.5, 0.4375, ((2, 8),))
    mix_bias = noise(arg_keys[4], (LAYERS, 2, BLOCKS, BLOCK), 0.5, 3.0, ((2, 8),))
    mix_second = noise(arg_keys[5], (LAYERS, 2, BLOCKS, BLOCK, BLOCK), (2 * BLOCK) ** -0.5, 0.4375, ((2, 8),))
    return {"field_in": field_in, "ln_gain": ln_gain, "ln_shift": ln_shift, "mix_first": mix_first, "mix_bias": mix_bias, "mix_second": mix_second}


norm_eps = 1e-05
shrink_level = 0.01

def trig_pair(length, freq_count):
    positions = jnp.arange(length, dtype=jnp.int32)
    freq_ids = jnp.arange(freq_count, dtype=jnp.int32)
    phase_ids = positions[:, None] * freq_ids[None, :] % length
    angles = phase_ids.astype(jnp.float32) * (2.0 * math.pi / length)
    norm_scale = 1.0 / math.sqrt(length)
    return ((jnp.cos(angles) * norm_scale).astype(jnp.bfloat16), (jnp.sin(angles) * norm_scale).astype(jnp.bfloat16))

def soft_shrink(values):
    return jnp.sign(values) * jnp.maximum(jnp.abs(values) - shrink_level, 0.0)

def reference(field_in, ln_gain, ln_shift, mix_first, mix_bias, mix_second):
    lon_cos, lon_sin = trig_pair(LON, MODES)
    lat_cos, lat_sin = trig_pair(LAT, LAT)
    cos_rows = lat_cos.astype(jnp.float32)
    sin_rows = lat_sin.astype(jnp.float32)
    mode_weight = jnp.where(jnp.arange(MODES) == 0, 1.0, 2.0).astype(jnp.float32)
    inv_cos = lon_cos.astype(jnp.float32) * mode_weight[None, :]
    inv_sin = lon_sin.astype(jnp.float32) * mode_weight[None, :]
    fwd_cos = lon_cos.astype(jnp.float32)
    fwd_sin = lon_sin.astype(jnp.float32)

    def block_filter(inputs):
        normed_block, first_w, first_b, second_w = inputs
        source = normed_block.astype(jnp.float32)
        lon_re = jnp.einsum('chw,wk->chk', source, fwd_cos).astype(jnp.bfloat16).astype(jnp.float32)
        lon_im = (-jnp.einsum('chw,wk->chk', source, fwd_sin)).astype(jnp.bfloat16).astype(jnp.float32)
        spec_re = (jnp.einsum('hj,chk->cjk', cos_rows, lon_re) + jnp.einsum('hj,chk->cjk', sin_rows, lon_im)).astype(jnp.bfloat16).astype(jnp.float32)
        spec_im = (jnp.einsum('hj,chk->cjk', cos_rows, lon_im) - jnp.einsum('hj,chk->cjk', sin_rows, lon_re)).astype(jnp.bfloat16).astype(jnp.float32)
        first_re = first_w[0].astype(jnp.float32)
        first_im = first_w[1].astype(jnp.float32)
        bias_f = first_b.astype(jnp.float32)
        hid_re = jax.nn.relu(jnp.einsum('cjk,cd->djk', spec_re, first_re) - jnp.einsum('cjk,cd->djk', spec_im, first_im) + bias_f[0][:, None, None])
        hid_im = jax.nn.relu(jnp.einsum('cjk,cd->djk', spec_im, first_re) + jnp.einsum('cjk,cd->djk', spec_re, first_im) + bias_f[1][:, None, None])
        hid_re = hid_re.astype(jnp.bfloat16).astype(jnp.float32)
        hid_im = hid_im.astype(jnp.bfloat16).astype(jnp.float32)
        second_re = second_w[0].astype(jnp.float32)
        second_im = second_w[1].astype(jnp.float32)
        mix_re = soft_shrink(jnp.einsum('cjk,cd->djk', hid_re, second_re) - jnp.einsum('cjk,cd->djk', hid_im, second_im))
        mix_im = soft_shrink(jnp.einsum('cjk,cd->djk', hid_im, second_re) + jnp.einsum('cjk,cd->djk', hid_re, second_im))
        mix_re = mix_re.astype(jnp.bfloat16).astype(jnp.float32)
        mix_im = mix_im.astype(jnp.bfloat16).astype(jnp.float32)
        back_re = (jnp.einsum('jh,cjk->chk', cos_rows, mix_re) - jnp.einsum('jh,cjk->chk', sin_rows, mix_im)).astype(jnp.bfloat16).astype(jnp.float32)
        back_im = (jnp.einsum('jh,cjk->chk', cos_rows, mix_im) + jnp.einsum('jh,cjk->chk', sin_rows, mix_re)).astype(jnp.bfloat16).astype(jnp.float32)
        return jnp.einsum('chk,wk->chw', back_re, inv_cos) - jnp.einsum('chk,wk->chw', back_im, inv_sin)
    row_pos = jnp.arange(LAT, dtype=jnp.float32)
    area_weights = jnp.cos((row_pos + 0.5) * (math.pi / LAT) - 0.5 * math.pi)[None, :, None]
    current = field_in
    source = field_in.astype(jnp.float32)
    target = jnp.sum(area_weights * source * source)
    for layer_idx in range(LAYERS):
        total_sum = lax.optimization_barrier(jnp.sum(source, axis=0))
        squares = lax.optimization_barrier(jnp.sum(source * source, axis=0))
        mean_val = total_sum / CH
        spread = squares / CH - mean_val * mean_val
        inv_std = lax.rsqrt(spread + norm_eps)
        gain_col = ln_gain[layer_idx].astype(jnp.float32)[:, None, None]
        shift_col = ln_shift[layer_idx].astype(jnp.float32)[:, None, None]
        normed = ((source - mean_val) * inv_std * gain_col + shift_col).astype(jnp.bfloat16)
        blocks_in = normed.reshape(BLOCKS, BLOCK, LAT, LON)
        first_w = jnp.moveaxis(mix_first[layer_idx], 1, 0)
        first_b = jnp.moveaxis(mix_bias[layer_idx], 1, 0)
        second_w = jnp.moveaxis(mix_second[layer_idx], 1, 0)
        spatial = lax.map(block_filter, (blocks_in, first_w, first_b, second_w)).reshape(CH, LAT, LON)
        summed = spatial + normed.astype(jnp.float32) + current.astype(jnp.float32)
        energy = jnp.sum(area_weights * summed * summed)
        current = (summed * jnp.sqrt(target / energy)).astype(jnp.bfloat16)
        source = current.astype(jnp.float32)
    return current
```

```python
import math

import jax
import jax.numpy as jnp
from jax import lax
from jax.experimental import pallas as pl
from jax.experimental.pallas import tpu as pltpu
from jax.sharding import Mesh
from jax.sharding import PartitionSpec as P

CH = ("ch_0", "ch_1")
LAT = ("lat_0", "lat_1")
MESH = pl.DeviceIdType.MESH

norm_eps = 1e-05
shrink_level = 0.01

F32 = jnp.float32
BF16 = jnp.bfloat16

N_LAT = 16
BAND = 24
CHN = 96
ROWS = CHN * BAND
LON = 768
LATS = N_LAT * BAND
CHUNKS = 3
KL = 8
ALL_CH = 768
PIECE = 12 * BAND

ORDER = [
    (1, 1), (3, 3), (2, 2), (1, 0), (3, 0), (0, 1), (0, 3), (1, 3), (3, 1),
    (2, 0), (0, 2), (1, 2), (3, 2), (2, 1), (2, 3),
]
CH_ORDER = [(1, 0), (3, 0), (1, 1), (3, 1), (2, 0), (2, 1), (0, 1)]


def trig(length, n, f):
    phase = n * f % length
    ang = phase.astype(F32) * (2.0 * math.pi / length)
    scale = 1.0 / math.sqrt(length)
    return jnp.cos(ang) * scale, jnp.sin(ang) * scale


def lon_table():
    row = jnp.arange(LON, dtype=jnp.int32)
    c = row // 256
    half = row // 128 % 2
    kk = row // 8 % 16
    q = half * 8 + row % 8
    mode = q * BAND + c * KL + kk % KL
    w = jnp.arange(LON, dtype=jnp.int32)
    cs, sn = trig(LON, mode[:, None], w[None, :])
    return jnp.where((kk < KL)[:, None], cs, -sn).astype(BF16).reshape(CHUNKS, 256, LON)


def lat_tables():
    n = jnp.arange(LATS, dtype=jnp.int32)
    cs, sn = trig(LATS, n[:, None], n[None, :])
    return cs.astype(BF16), sn.astype(BF16)


def kernel(
    x_ref, tb_ref, cl_ref, sl_ref, a1_ref, b1_ref, a2_ref, area_ref, gain_ref, shift_ref,
    o_ref,
    V, N, TF, TI, LF, LI, SF, RF, SB, RB, G, R, SP, MX,
    ST, RS, RED, AG, ES, EB, TG, MI,
    fs, fr, bs, br, rss, rsr, ags, agr, es, er,
):
    y = lax.axis_index("lat_0")
    z = lax.axis_index("lat_1")
    cx = lax.axis_index("ch_0")
    ck = lax.axis_index("ch_1")
    me = y * 4 + z
    mc = cx * 2 + ck

    def lat_to(a, b):
        yy = lax.rem(y + a, 4)
        zz = lax.rem(z + b, 4)
        return {"lat_0": yy, "lat_1": zz}, yy * 4 + zz

    def ch_to(a, b):
        xx = lax.rem(cx + a, 4)
        kk = lax.rem(ck + b, 2)
        return {"ch_0": xx, "ch_1": kk}, xx * 2 + kk

    bar = pltpu.get_barrier_semaphore()
    for a, b in ORDER:
        pl.semaphore_signal(bar, 1, device_id=lat_to(a, b)[0], device_id_type=MESH)
    for a, b in CH_ORDER:
        pl.semaphore_signal(bar, 1, device_id=ch_to(a, b)[0], device_id_type=MESH)
    pl.semaphore_wait(bar, len(ORDER) + len(CH_ORDER))

    def rcopy(src, dst, ss, rr, dev):
        return pltpu.make_async_remote_copy(
            src_ref=src, dst_ref=dst, send_sem=ss, recv_sem=rr, device_id=dev, device_id_type=MESH
        )

    def exchange_start(sb, rb, ss, rr, c):
        for a, b in ORDER:
            dev, q = lat_to(a, b)
            rcopy(sb.at[c, q], rb.at[c, me], ss.at[c, q], rr.at[c, me], dev).start()
        rb[c, me] = sb[c, me]

    def exchange_recv(sb, rb, ss, rr, c):
        for a, b in ORDER:
            dev, p = lat_to(4 - a, 4 - b)
            rcopy(sb.at[c, p], rb.at[c, p], ss.at[c, p], rr.at[c, p], dev).wait_recv()

    def exchange_sent(sb, rb, ss, rr, c):
        for a, b in ORDER:
            dev, q = lat_to(a, b)
            rcopy(sb.at[c, q], rb.at[c, me], ss.at[c, q], rr.at[c, me], dev).wait_send()

    def partial_sums(load):
        def step(i, carry):
            s1, s2 = carry
            for v in load(i):
                s1 = s1 + v
                s2 = s2 + v * v
            return s1, s2

        zero = jnp.zeros((BAND, LON), F32)
        s1, s2 = lax.fori_loop(0, CHN // 2, step, (zero, zero))
        for hb in range(3):
            for lb in range(6):
                ST[hb * 6 + lb] = s1[8 * hb : 8 * hb + 8, 128 * lb : 128 * lb + 128]
                ST[18 + hb * 6 + lb] = s2[8 * hb : 8 * hb + 8, 128 * lb : 128 * lb + 128]
        for t in range(36, 40):
            ST[t] = jnp.zeros((8, 128), F32)
        e = jnp.zeros((8, 128), F32)
        for hb in range(3):
            for lb in range(6):
                e = e + ST[18 + hb * 6 + lb] * area_ref[8 * hb : 8 * hb + 8, :]
        ES[...] = e

    def load_input(i):
        xx = x_ref[pl.ds(pl.multiple_of(i * 48, 48), 48), :].astype(F32)
        V[pl.ds(pl.multiple_of(i * 48, 48), 48), :] = xx
        return xx[0:24], xx[24:48]

    def load_v(i):
        return (
            V[pl.ds(pl.multiple_of(i * 48, 48), 24), :],
            V[pl.ds(pl.multiple_of(i * 48 + 24, 24), 24), :],
        )

    def e_copy(a, b):
        dev, q = lat_to(a, b)
        return rcopy(ES, EB.at[me], es.at[q], er.at[me], dev)

    def e_from(a, b):
        dev, p = lat_to(4 - a, 4 - b)
        return rcopy(ES, EB.at[p], es.at[p], er.at[p], dev)

    def rs_copy(a, b):
        dev, d = ch_to(a, b)
        return rcopy(ST.at[pl.ds(5 * d, 5)], RS.at[mc], rss.at[d], rsr.at[mc], dev)

    def rs_from(a, b):
        dev, d = ch_to(4 - a, 2 - b)
        return rcopy(ST.at[pl.ds(5 * d, 5)], RS.at[d], rss.at[d], rsr.at[d], dev)

    def ag_copy(a, b):
        dev, d = ch_to(a, b)
        return rcopy(RED, AG.at[mc], ags.at[d], agr.at[mc], dev)

    def ag_from(a, b):
        dev, d = ch_to(4 - a, 2 - b)
        return rcopy(RED, AG.at[d], ags.at[d], agr.at[d], dev)

    def exchange_stats(between):
        for a, b in CH_ORDER:
            rs_copy(a, b).start()
        for a, b in ORDER:
            e_copy(a, b).start()
        RS[mc] = ST[pl.ds(5 * mc, 5)]
        EB[me] = ES[...]
        between()
        for a, b in CH_ORDER:
            rs_from(a, b).wait_recv()
        tot = RS[0]
        for d in range(1, 8):
            tot = tot + RS[d]
        RED[0:5] = tot
        for a, b in ORDER:
            e_from(a, b).wait_recv()
        e = EB[0]
        for p in range(1, N_LAT):
            e = e + EB[p]
        RED[5] = e
        for a, b in CH_ORDER:
            ag_copy(a, b).start()
        AG[mc] = RED[...]
        for a, b in CH_ORDER:
            ag_from(a, b).wait_recv()
        for a, b in CH_ORDER:
            rs_copy(a, b).wait_send()
            ag_copy(a, b).wait_send()
        for a, b in ORDER:
            e_copy(a, b).wait_send()
        e = AG[0, 5]
        for d in range(1, 8):
            e = e + AG[d, 5]
        e = jnp.sum(e, axis=0, keepdims=True)
        e = jnp.sum(e, axis=1, keepdims=True)
        return jnp.broadcast_to(e, (8, 128))

    def lane_masks():
        lane = lax.broadcasted_iota(jnp.int32, (48, 128), 1) & 7
        return [lane == s for s in range(8)]

    def block_swap(parts, masks):
        rolled = [p if r == 0 else pltpu.roll(p, r, 1) for r, p in enumerate(parts)]
        out = []
        for q in range(8):
            acc = rolled[-q % 8]
            for s in range(1, 8):
                acc = jnp.where(masks[s], rolled[(s - q) % 8], acc)
            out.append(acc if q == 0 else pltpu.roll(acc, 128 - q, 1))
        return out

    def forward_chunk(c, _):
        def step(i, _):
            base = pl.multiple_of(i * 384, 384)
            R[...] = jnp.dot(N[pl.ds(base, 384), :], TF[c], preferred_element_type=F32)
            masks = lane_masks()
            for half in range(2):
                hs = slice(128 * half, 128 * half + 128)
                parts = [
                    jnp.concatenate(
                        [R[24 * r : 24 * r + 24, hs], R[192 + 24 * r : 216 + 24 * r, hs]], axis=0
                    )
                    for r in range(8)
                ]
                for q, piece in enumerate(block_swap(parts, masks)):
                    SF[c, 8 * half + q, pl.ds(pl.multiple_of(i * 48, 48), 48), :] = piece.astype(BF16)
            return 0

        lax.fori_loop(0, 6, step, 0)
        exchange_start(SF, RF, fs, fr, c)
        return 0

    def middle_chunk(l, c):
        exchange_recv(SF, RF, fs, fr, c)

        def gather(i, _):
            rows = pl.ds(pl.multiple_of(i * 48, 48), 48)
            got = [RF[c, p, rows, :].astype(F32) for p in range(N_LAT)]
            for j in range(2):
                blk = jnp.concatenate([g[24 * j : 24 * j + 24] for g in got], axis=0)
                t = blk.T.reshape(16, 8, LATS)
                G[:, pl.ds(pl.multiple_of(i * 16 + 8 * j, 8), 8), :] = t
            return 0

        lax.fori_loop(0, 6, gather, 0)

        def mix(b, _):
            g_re = G[pl.ds(4 * b, 4)].reshape(384, LATS).astype(BF16)
            g_im = G[pl.ds(8 + 4 * b, 4)].reshape(384, LATS).astype(BF16)
            SP[...] = jnp.dot(
                jnp.concatenate([g_re, g_im], axis=1), LF[...], preferred_element_type=F32
            ).astype(BF16)

            for k in range(4):
                rows = slice(96 * k, 96 * k + 96)
                both = jnp.concatenate([SP[rows, 0:LATS], SP[rows, LATS:]], axis=0)
                hid = jnp.dot(a1_ref[l], both, preferred_element_type=F32) + b1_ref[l]
                hid = jnp.maximum(hid, 0.0).astype(BF16)
                m = jnp.dot(a2_ref[l], hid, preferred_element_type=F32)
                m = (m - jnp.clip(m, -shrink_level, shrink_level)).astype(BF16)
                MX[rows, 0:LATS] = m[0:96]
                MX[rows, LATS:] = m[96:192]
            back = jnp.dot(MX[...], LI[...], preferred_element_type=F32)
            G[pl.ds(4 * b, 4)] = back[:, 0:LATS].reshape(4, CHN, LATS)
            G[pl.ds(8 + 4 * b, 4)] = back[:, LATS:].reshape(4, CHN, LATS)
            return 0

        lax.fori_loop(0, 2, mix, 0)

        def scatter(i, _):
            ts = []
            for j in range(2):
                blk = G[:, pl.ds(pl.multiple_of(i * 16 + 8 * j, 8), 8), :].reshape(128, LATS)
                ts.append(blk.T)
            for p in range(N_LAT):
                piece = jnp.concatenate([t[24 * p : 24 * p + 24] for t in ts], axis=0)
                SB[c, p, pl.ds(pl.multiple_of(i * 48, 48), 48), :] = piece.astype(BF16)
            return 0

        lax.fori_loop(0, 6, scatter, 0)
        exchange_start(SB, RB, bs, br, c)

    def backward_chunk(c, _):
        exchange_recv(SB, RB, bs, br, c)

        def step(i, _):
            rows = pl.ds(pl.multiple_of(i * 48, 48), 48)
            masks = lane_masks()
            for half in range(2):
                hs = slice(128 * half, 128 * half + 128)
                parts = [RB[c, 8 * half + q, rows, :].astype(F32) for q in range(8)]
                for r, piece in enumerate(block_swap(parts, masks)):
                    R[24 * r : 24 * r + 24, hs] = piece[0:24]
                    R[192 + 24 * r : 216 + 24 * r, hs] = piece[24:48]
            base = pl.multiple_of(i * 384, 384)
            V[pl.ds(base, 384), :] += jnp.dot(
                R[...].astype(BF16), TI[c], preferred_element_type=F32
            )
            return 0

        lax.fori_loop(0, 6, step, 0)
        return 0

    def set_tables():
        row = lax.broadcasted_iota(jnp.int32, (256, LON), 0)
        for c in range(CHUNKS):
            t = tb_ref[c].astype(F32)
            TF[c] = t.T.astype(BF16)
            twice = t * 2.0
            TI[c] = (jnp.where(row == 0, t, twice) if c == 0 else twice).astype(BF16)
        cl = cl_ref[...]
        sl = sl_ref[...]
        LF[0:LATS, 0:LATS] = cl
        LF[0:LATS, LATS:] = -sl
        LF[LATS:, 0:LATS] = sl
        LF[LATS:, LATS:] = cl
        LI[0:LATS, 0:LATS] = cl
        LI[0:LATS, LATS:] = sl
        LI[LATS:, 0:LATS] = -sl
        LI[LATS:, LATS:] = cl

    def normalize(l, scale):
        for hb in range(3):
            for lb in range(6):
                t = hb * 6 + lb
                mean = AG[t // 5, t % 5] * scale * (1.0 / ALL_CH)
                u = t + 18
                spread = AG[u // 5, u % 5] * (scale * scale) * (1.0 / ALL_CH) - mean * mean
                MI[0, 8 * hb : 8 * hb + 8, 128 * lb : 128 * lb + 128] = mean
                MI[1, 8 * hb : 8 * hb + 8, 128 * lb : 128 * lb + 128] = lax.rsqrt(spread + norm_eps)
        srow = scale[0:1, 0:1]

        def step(i, _):
            base = pl.multiple_of(i * 48, 48)
            for lb in range(2):
                ls = slice(384 * lb, 384 * lb + 384)
                mean = MI[0, :, ls]
                inv = MI[1, :, ls]
                both = []
                for j in range(2):
                    rows = pl.ds(pl.multiple_of(i * 48 + 24 * j, 24), 24)
                    cur = (V[rows, ls] * srow).astype(BF16).astype(F32)
                    nrm = (cur - mean) * inv * gain_ref[l, 2 * i + j] + shift_ref[l, 2 * i + j]
                    nrm = nrm.astype(BF16)
                    V[rows, ls] = cur + nrm.astype(F32)
                    both.append(nrm.astype(F32))
                N[pl.ds(base, 48), ls] = jnp.concatenate(both, axis=0).astype(BF16)
            return 0

        lax.fori_loop(0, CHN // 2, step, 0)

    def layer(l, scale):
        normalize(l, scale)
        lax.fori_loop(0, CHUNKS, forward_chunk, 0)

        def mid(c, _):
            middle_chunk(l, c)
            return 0

        lax.fori_loop(0, CHUNKS, mid, 0)
        lax.fori_loop(0, CHUNKS, backward_chunk, 0)

        def sent(c, _):
            exchange_sent(SF, RF, fs, fr, c)
            exchange_sent(SB, RB, bs, br, c)
            return 0

        lax.fori_loop(0, CHUNKS, sent, 0)
        partial_sums(load_v)
        energy = exchange_stats(lambda: None)
        return jnp.sqrt(TG[...] / energy)

    partial_sums(load_input)
    TG[...] = exchange_stats(set_tables)
    scale = lax.fori_loop(0, 2, layer, jnp.ones((8, 128), F32))

    srow = scale[0:1, 0:1]

    def finish(i, _):
        rows = pl.ds(pl.multiple_of(i * 48, 48), 48)
        o_ref[rows, :] = (V[rows, :] * srow).astype(BF16)
        return 0

    lax.fori_loop(0, CHN // 2, finish, 0)


def complex_block(w):
    re = jnp.swapaxes(w[:, 0], 1, 2)
    im = jnp.swapaxes(w[:, 1], 1, 2)
    top = jnp.concatenate([re, -im], axis=2)
    low = jnp.concatenate([im, re], axis=2)
    return jnp.concatenate([top, low], axis=1)


def per_device(field_in, ln_gain, ln_shift, mix_first, mix_bias, mix_second):
    layers = mix_first.shape[0]
    a1 = complex_block(mix_first[:, :, 0])
    a2 = complex_block(mix_second[:, :, 0])
    b1 = mix_bias[:, :, 0].astype(F32).reshape(layers, 2 * CHN, 1)
    cl, sl = lat_tables()
    row = (lax.axis_index(LAT) * BAND + jnp.arange(BAND, dtype=jnp.int32)).astype(F32)
    area = jnp.cos((row + 0.5) * (math.pi / LATS) - 0.5 * math.pi)
    area = jnp.broadcast_to(area[:, None], (BAND, 128))
    vm = pl.BlockSpec(memory_space=pltpu.VMEM)
    sm = pl.BlockSpec(memory_space=pltpu.SMEM)
    dma = pltpu.SemaphoreType.DMA
    out = pl.pallas_call(
        kernel,
        out_shape=jax.ShapeDtypeStruct((ROWS, LON), BF16),
        in_specs=[vm] * 8 + [sm] * 2,
        out_specs=vm,
        scratch_shapes=[
            pltpu.VMEM((ROWS, LON), F32),
            pltpu.VMEM((ROWS, LON), BF16),
            pltpu.VMEM((CHUNKS, LON, 256), BF16),
            pltpu.VMEM((CHUNKS, 256, LON), BF16),
            pltpu.VMEM((2 * LATS, 2 * LATS), BF16),
            pltpu.VMEM((2 * LATS, 2 * LATS), BF16),
            pltpu.VMEM((CHUNKS, N_LAT, PIECE, 128), BF16),
            pltpu.VMEM((CHUNKS, N_LAT, PIECE, 128), BF16),
            pltpu.VMEM((CHUNKS, N_LAT, PIECE, 128), BF16),
            pltpu.VMEM((CHUNKS, N_LAT, PIECE, 128), BF16),
            pltpu.VMEM((16, CHN, LATS), F32),
            pltpu.VMEM((384, 256), F32),
            pltpu.VMEM((384, 2 * LATS), BF16),
            pltpu.VMEM((384, 2 * LATS), BF16),
            pltpu.VMEM((40, 8, 128), F32),
            pltpu.VMEM((8, 5, 8, 128), F32),
            pltpu.VMEM((6, 8, 128), F32),
            pltpu.VMEM((8, 6, 8, 128), F32),
            pltpu.VMEM((8, 128), F32),
            pltpu.VMEM((N_LAT, 8, 128), F32),
            pltpu.VMEM((8, 128), F32),
            pltpu.VMEM((2, BAND, LON), F32),
            dma((CHUNKS, N_LAT)),
            dma((CHUNKS, N_LAT)),
            dma((CHUNKS, N_LAT)),
            dma((CHUNKS, N_LAT)),
            dma((8,)),
            dma((8,)),
            dma((8,)),
            dma((8,)),
            dma((N_LAT,)),
            dma((N_LAT,)),
        ],
        compiler_params=pltpu.CompilerParams(
            collective_id=0, has_side_effects=True, vmem_limit_bytes=60 * 1024 * 1024
        ),
    )(
        field_in.reshape(ROWS, LON), lon_table(), cl, sl, a1, b1, a2, area, ln_gain, ln_shift
    )
    return out.reshape(CHN, BAND, LON)


def solution(mesh):
    finer = Mesh(mesh.devices.reshape(4, 4, 4, 2), ("lat_0", "lat_1", "ch_0", "ch_1"))
    in_specs = (
        P(CH, LAT, None),
        P(None, CH),
        P(None, CH),
        P(None, None, CH, None, None),
        P(None, None, CH, None),
        P(None, None, CH, None, None),
    )
    return jax.shard_map(
        per_device, mesh=finer, in_specs=in_specs, out_specs=P(CH, LAT, None), check_vma=False
    )
```

```python
import math

import jax
import jax.numpy as jnp
import numpy as np
from jax import lax
from jax.experimental import pallas as pl
from jax.experimental.pallas import tpu as pltpu
from jax.sharding import Mesh
from jax.sharding import PartitionSpec as P

CH = ("ch_0", "ch_1")
LAT = ("lat_0", "lat_1")
MESH = pl.DeviceIdType.MESH

norm_eps = 1e-05
shrink_level = 0.01

F32 = jnp.float32
BF16 = jnp.bfloat16

N_LAT = 16
BAND = 24
CHN = 96
ROWS = CHN * BAND
LON = 768
LATS = N_LAT * BAND
CHUNKS = 3
KL = 8
ALL_CH = 768
PIECE = 12 * BAND

ORDER = [
    (1, 1), (3, 3), (2, 2), (1, 0), (3, 0), (0, 1), (0, 3), (1, 3), (3, 1),
    (2, 0), (0, 2), (1, 2), (3, 2), (2, 1), (2, 3),
]
CH_ORDER = [(1, 0), (3, 0), (1, 1), (3, 1), (2, 0), (2, 1), (0, 1)]


NSUB = 3
SUBSTEPS = 6 // NSUB
SUBROWS = PIECE // NSUB


def trig(length, n, f):
    ang = (n * f % length) * (2.0 * math.pi / length)
    scale = 1.0 / math.sqrt(length)
    return np.cos(ang) * scale, np.sin(ang) * scale


def lon_table():
    row = np.arange(LON)
    kk = row // 8 % 16
    q = row // 128 % 2 * 8 + row % 8
    mode = q * BAND + row // 256 * KL + kk % KL
    cs, sn = trig(LON, mode[:, None], np.arange(LON)[None, :])
    return np.where((kk < KL)[:, None], cs, -sn).reshape(CHUNKS, 256, LON).astype(BF16)


def lat_tables():
    n = np.arange(LATS)
    cs, sn = trig(LATS, n[:, None], n[None, :])
    return np.stack([cs, sn]).astype(BF16)


def area_table():
    row = np.arange(LATS, dtype=np.float32).reshape(N_LAT, BAND, 1)
    area = np.cos((row + 0.5) * (math.pi / LATS) - 0.5 * math.pi)
    return np.broadcast_to(area, (N_LAT, BAND, 128)).astype(np.float32)


def kernel(
    x_hbm, tb_hbm, cs_hbm, w1_ref, b_ref, w2_ref, area_ref, gain_ref, shift_ref,
    o_ref,
    X, TB, CS, V, N, TF, TI, LF, LI, SF, RF, SB, RB, G, R, SP, MX, AW, A1, A2, BT, B1,
    PS, ST, RS, RED, AG, AF, ES, EB, TC, EN, MI,
    xs, ts, fs, fr, bs, br, rss, rsr, ags, agr, afs, afr, es, er,
):
    y = lax.axis_index("lat_0")
    z = lax.axis_index("lat_1")
    cx = lax.axis_index("ch_0")
    ck = lax.axis_index("ch_1")
    me = y * 4 + z
    mc = cx * 2 + ck

    def x_copy(i):
        rows = pl.ds(pl.multiple_of(i * 384, 384), 384)
        return pltpu.make_async_copy(x_hbm.at[rows], X.at[rows], xs.at[i])

    for i in range(6):
        x_copy(i).start()
    pltpu.make_async_copy(tb_hbm, TB, ts.at[0]).start()
    pltpu.make_async_copy(cs_hbm, CS, ts.at[1]).start()

    def lat_to(a, b):
        yy = lax.rem(y + a, 4)
        zz = lax.rem(z + b, 4)
        return {"lat_0": yy, "lat_1": zz}, yy * 4 + zz

    def ch_to(a, b):
        xx = lax.rem(cx + a, 4)
        kk = lax.rem(ck + b, 2)
        return {"ch_0": xx, "ch_1": kk}, xx * 2 + kk

    bar = pltpu.get_barrier_semaphore()
    for a, b in ORDER:
        pl.semaphore_signal(bar, 1, device_id=lat_to(a, b)[0], device_id_type=MESH)
    for a, b in CH_ORDER:
        pl.semaphore_signal(bar, 1, device_id=ch_to(a, b)[0], device_id_type=MESH)

    def rcopy(src, dst, ss, rr, dev):
        return pltpu.make_async_remote_copy(
            src_ref=src, dst_ref=dst, send_sem=ss, recv_sem=rr, device_id=dev, device_id_type=MESH
        )

    def unit_start(sb, rb, ss, rr, c, u):
        for a, b in ORDER:
            dev, q = lat_to(a, b)
            rcopy(sb.at[c, u, q], rb.at[c, u, me], ss.at[c, u], rr.at[c, u], dev).start()
        rb[c, u, me] = sb[c, u, me]

    def unit_whole(sb, rb, ss, rr, c, u):
        peers = pl.ds(0, N_LAT - 1)
        dev = lat_to(1, 0)[0]
        return rcopy(sb.at[c, u, peers], rb.at[c, u, peers], ss.at[c, u], rr.at[c, u], dev)

    def stats_out():
        e = jnp.zeros((8, 128), F32)
        for hb in range(3):
            for lb in range(6):
                t = hb * 6 + lb
                rows, lanes = slice(8 * hb, 8 * hb + 8), slice(128 * lb, 128 * lb + 128)
                sq = PS[1, rows, lanes]
                ST[t] = PS[0, rows, lanes]
                ST[18 + t] = sq
                e = e + sq * area_ref[me, rows, :]
        ES[...] = e

    def e_copy(a, b):
        dev, q = lat_to(a, b)
        return rcopy(ES, EB.at[me], es.at[q], er.at[me], dev)

    def e_from(a, b):
        dev, p = lat_to(4 - a, 4 - b)
        return rcopy(ES, EB.at[p], es.at[p], er.at[p], dev)

    def rs_copy(a, b):
        dev, d = ch_to(a, b)
        return rcopy(ST.at[pl.ds(5 * d, 5)], RS.at[mc], rss.at[d], rsr.at[mc], dev)

    def rs_from(a, b):
        dev, d = ch_to(4 - a, 2 - b)
        return rcopy(ST.at[pl.ds(5 * d, 5)], RS.at[d], rss.at[d], rsr.at[d], dev)

    def ag_copy(a, b, part):
        dev, d = ch_to(a, b)
        return rcopy(RED.at[part], AG.at[mc, part], ags.at[d], agr.at[mc], dev)

    def ag_from(a, b, part):
        dev, d = ch_to(4 - a, 2 - b)
        return rcopy(RED.at[part], AG.at[d, part], ags.at[d], agr.at[d], dev)

    def rs_start():
        for a, b in CH_ORDER:
            rs_copy(a, b).start()
        RS[mc] = ST[pl.ds(5 * mc, 5)]

    def e_start():
        for a, b in ORDER:
            e_copy(a, b).start()
        EB[me] = ES[...]

    def rs_sum():
        for a, b in CH_ORDER:
            rs_from(a, b).wait_recv()
        tot = RS[0]
        for d in range(1, 8):
            tot = tot + RS[d]
        RED[0:5] = tot

    def e_sum():
        for a, b in ORDER:
            e_from(a, b).wait_recv()
        e = EB[0]
        for p in range(1, N_LAT):
            e = e + EB[p]
        return e

    def ag_start(part):
        for a, b in CH_ORDER:
            ag_copy(a, b, part).start()
        AG[mc, part] = RED[part]

    def ag_wait(part):
        for a, b in CH_ORDER:
            ag_from(a, b, part).wait_recv()

    def rs_sent():
        for a, b in CH_ORDER:
            rs_copy(a, b).wait_send()

    def ag_sent(part):
        for a, b in CH_ORDER:
            ag_copy(a, b, part).wait_send()

    def e_sent():
        for a, b in ORDER:
            e_copy(a, b).wait_send()

    def af_copy(a, b):
        dev, d = ch_to(a, b)
        return rcopy(RED.at[5], AF.at[mc], afs.at[d], afr.at[mc], dev)

    def af_from(a, b):
        dev, d = ch_to(4 - a, 2 - b)
        return rcopy(RED.at[5], AF.at[d], afs.at[d], afr.at[d], dev)

    def over_channels(tiles):
        e = tiles[0]
        for d in range(1, 8):
            e = e + tiles[d]
        e = jnp.sum(e, axis=0, keepdims=True)
        e = jnp.sum(e, axis=1, keepdims=True)
        return jnp.broadcast_to(e, (8, 128))

    def lane_masks():
        lane = lax.broadcasted_iota(jnp.int32, (48, 128), 1) & 7
        return [lane == s for s in range(8)]

    def block_swap(parts, masks):
        rolled = [p if r == 0 else pltpu.roll(p, r, 1) for r, p in enumerate(parts)]
        out = []
        for q in range(8):
            acc = rolled[-q % 8]
            for s in range(1, 8):
                acc = jnp.where(masks[s], rolled[(s - q) % 8], acc)
            out.append(acc if q == 0 else pltpu.roll(acc, 128 - q, 1))
        return out

    def rows_of(ii):
        return pl.ds(pl.multiple_of(ii * 48, 48), 48)

    def forward_step(c, u, ii):
        base = pl.multiple_of((u * SUBSTEPS + ii) * 384, 384)
        R[...] = jnp.dot(N[pl.ds(base, 384), :], TF[c], preferred_element_type=F32)
        masks = lane_masks()
        for half in range(2):
            hs = slice(128 * half, 128 * half + 128)
            parts = [
                jnp.concatenate(
                    [R[24 * r : 24 * r + 24, hs], R[192 + 24 * r : 216 + 24 * r, hs]], axis=0
                )
                for r in range(8)
            ]
            for q, piece in enumerate(block_swap(parts, masks)):
                SF[c, u, 8 * half + q, rows_of(ii), :] = piece.astype(BF16)

    def normalize_step(l, srow, i):
        def pair(j, _):
            base = i * 384 + j * 48
            ch = i * 16 + j * 2
            for lb in range(2):
                ls = slice(384 * lb, 384 * lb + 384)
                mean = MI[0, :, ls]
                inv = MI[1, :, ls]
                both = []
                for t in range(2):
                    rows = pl.ds(pl.multiple_of(base + 24 * t, 24), 24)
                    cur = (V[rows, ls] * srow).astype(BF16).astype(F32)
                    nrm = (cur - mean) * inv * gain_ref[l, ch + t] + shift_ref[l, ch + t]
                    nrm = nrm.astype(BF16).astype(F32)
                    V[rows, ls] = cur + nrm
                    both.append(nrm)
                N[pl.ds(pl.multiple_of(base, 48), 48), ls] = jnp.concatenate(both, axis=0).astype(BF16)
            return 0

        lax.fori_loop(0, 8, pair, 0)

    def forward_first(l, srow):
        def unit(u, _):
            def step(ii, _):
                normalize_step(l, srow, u * SUBSTEPS + ii)
                forward_step(0, u, ii)
                return 0

            lax.fori_loop(0, SUBSTEPS, step, 0)
            unit_start(SF, RF, fs, fr, 0, u)
            return 0

        lax.fori_loop(0, NSUB, unit, 0)

    def forward_rest():
        def unit(n, _):
            c = n // NSUB
            u = n % NSUB

            def step(ii, _):
                forward_step(c, u, ii)
                return 0

            lax.fori_loop(0, SUBSTEPS, step, 0)
            unit_start(SF, RF, fs, fr, c, u)
            return 0

        lax.fori_loop(NSUB, CHUNKS * NSUB, unit, 0)

    def middle_chunk(l, c):
        def gather_unit(u, _):
            unit_whole(SF, RF, fs, fr, c, u).wait_recv()

            def gather(ii, _):
                i = u * SUBSTEPS + ii
                got = [RF[c, u, p, rows_of(ii), :].astype(F32) for p in range(N_LAT)]
                for j in range(2):
                    blk = jnp.concatenate([g[24 * j : 24 * j + 24] for g in got], axis=0)
                    t = blk.T.reshape(16, 8, LATS)
                    G[:, pl.ds(pl.multiple_of(i * 16 + 8 * j, 8), 8), :] = t
                return 0

            lax.fori_loop(0, SUBSTEPS, gather, 0)
            return 0

        lax.fori_loop(0, NSUB, gather_unit, 0)

        def mix(b, _):
            g_re = G[pl.ds(4 * b, 4)].reshape(384, LATS).astype(BF16)
            g_im = G[pl.ds(8 + 4 * b, 4)].reshape(384, LATS).astype(BF16)
            SP[...] = jnp.dot(
                jnp.concatenate([g_re, g_im], axis=1), LF[...], preferred_element_type=F32
            ).astype(BF16)
            bias = jnp.concatenate([B1[l]] * 3, axis=1)
            for k in range(4):
                rows = slice(96 * k, 96 * k + 96)
                both = jnp.concatenate([SP[rows, 0:LATS], SP[rows, LATS:]], axis=0)
                hid = jnp.dot(A1[l], both, preferred_element_type=F32) + bias
                hid = jnp.maximum(hid, 0.0).astype(BF16)
                m = jnp.dot(A2[l], hid, preferred_element_type=F32)
                m = (m - jnp.clip(m, -shrink_level, shrink_level)).astype(BF16)
                MX[rows, 0:LATS] = m[0:96]
                MX[rows, LATS:] = m[96:192]
            back = jnp.dot(MX[...], LI[...], preferred_element_type=F32)
            G[pl.ds(4 * b, 4)] = back[:, 0:LATS].reshape(4, CHN, LATS)
            G[pl.ds(8 + 4 * b, 4)] = back[:, LATS:].reshape(4, CHN, LATS)
            return 0

        lax.fori_loop(0, 2, mix, 0)

        def scatter_unit(u, _):
            def scatter(ii, _):
                i = u * SUBSTEPS + ii
                ts = []
                for j in range(2):
                    blk = G[:, pl.ds(pl.multiple_of(i * 16 + 8 * j, 8), 8), :].reshape(128, LATS)
                    ts.append(blk.T)
                for p in range(N_LAT):
                    piece = jnp.concatenate([t[24 * p : 24 * p + 24] for t in ts], axis=0)
                    SB[c, u, p, rows_of(ii), :] = piece.astype(BF16)
                return 0

            lax.fori_loop(0, SUBSTEPS, scatter, 0)
            unit_start(SB, RB, bs, br, c, u)
            return 0

        lax.fori_loop(0, NSUB, scatter_unit, 0)

    def backward_unit(c, u, last):
        unit_whole(SB, RB, bs, br, c, u).wait_recv()

        def step(ii, _):
            masks = lane_masks()
            for half in range(2):
                hs = slice(128 * half, 128 * half + 128)
                parts = [RB[c, u, 8 * half + q, rows_of(ii), :].astype(F32) for q in range(8)]
                for r, piece in enumerate(block_swap(parts, masks)):
                    R[24 * r : 24 * r + 24, hs] = piece[0:24]
                    R[192 + 24 * r : 216 + 24 * r, hs] = piece[24:48]
            rows = pl.ds(pl.multiple_of((u * SUBSTEPS + ii) * 384, 384), 384)
            v = V[rows, :] + jnp.dot(R[...].astype(BF16), TI[c], preferred_element_type=F32)
            V[rows, :] = v
            if last:
                v = v.reshape(16, BAND, LON)
                PS[0] += jnp.sum(v, axis=0)
                PS[1] += jnp.sum(v * v, axis=0)
            return 0

        lax.fori_loop(0, SUBSTEPS, step, 0)

    def set_tables():
        pltpu.make_async_copy(tb_hbm, TB, ts.at[0]).wait()
        pltpu.make_async_copy(cs_hbm, CS, ts.at[1]).wait()
        row = lax.broadcasted_iota(jnp.int32, (256, LON), 0)
        for c in range(CHUNKS):
            t = TB[c].astype(F32)
            TF[c] = t.T.astype(BF16)
            twice = t * 2.0
            TI[c] = (jnp.where(row == 0, t, twice) if c == 0 else twice).astype(BF16)
        cl = CS[0]
        sl = CS[1]
        LF[0:LATS, 0:LATS] = cl
        LF[0:LATS, LATS:] = -sl
        LF[LATS:, 0:LATS] = sl
        LF[LATS:, LATS:] = cl
        LI[0:LATS, 0:LATS] = cl
        LI[0:LATS, LATS:] = sl
        LI[LATS:, 0:LATS] = -sl
        LI[LATS:, LATS:] = cl
        AW[...] = jnp.zeros((256, 256), F32)
        BT[...] = jnp.zeros((128, 128), F32)
        for l in range(2):
            for w_ref, a_ref in ((w1_ref, A1), (w2_ref, A2)):
                re = w_ref[l, 0].astype(F32)
                im = w_ref[l, 1].astype(F32)
                AW[0:96, 0:192] = jnp.concatenate([re, im], axis=1)
                AW[96:192, 0:192] = jnp.concatenate([-im, re], axis=1)
                a_ref[l] = AW[...].T[0:192, 0:192].astype(BF16)
            for part in range(2):
                BT[:, 0:96] = jnp.broadcast_to(b_ref[l, part : part + 1, :].astype(F32), (128, 96))
                B1[l, 96 * part : 96 * part + 96, :] = BT[...].T[0:96, :]

    def set_mean_inv(scale):
        for hb in range(3):
            for lb in range(6):
                t = hb * 6 + lb
                u = t + 18
                mean = AG[t // 5, t % 5] * scale * (1.0 / ALL_CH)
                spread = AG[u // 5, u % 5] * (scale * scale) * (1.0 / ALL_CH) - mean * mean
                MI[0, 8 * hb : 8 * hb + 8, 128 * lb : 128 * lb + 128] = mean
                MI[1, 8 * hb : 8 * hb + 8, 128 * lb : 128 * lb + 128] = lax.rsqrt(spread + norm_eps)

    five, seven = pl.ds(0, 5), pl.ds(0, 7)

    zero = jnp.zeros((BAND, LON), F32)
    for t in range(36, 40):
        ST[t] = jnp.zeros((8, 128), F32)

    def first_block(i, carry):
        x_copy(i).wait()

        def pair(j, carry):
            s1, s2 = carry
            rows = pl.ds(pl.multiple_of(i * 384 + j * 48, 48), 48)
            xx = X[rows, :].astype(F32)
            V[rows, :] = xx
            for t in range(2):
                v = xx[24 * t : 24 * t + 24]
                s1 = s1 + v
                s2 = s2 + v * v
            return s1, s2

        return lax.fori_loop(0, 8, pair, carry)

    s1, s2 = lax.fori_loop(0, 6, first_block, (zero, zero))
    PS[0] = s1
    PS[1] = s2
    stats_out()
    pl.semaphore_wait(bar, len(ORDER) + len(CH_ORDER))
    rs_start()
    e_start()
    set_tables()
    rs_sum()
    ag_start(five)
    TC[...] = e_sum()
    ag_wait(five)
    rs_sent()
    ag_sent(five)
    e_sent()

    def layer(l, scale):
        set_mean_inv(scale)
        srow = scale[0:1, 0:1]
        forward_first(l, srow)
        forward_rest()

        def mid(c, _):
            middle_chunk(l, c)
            return 0

        lax.fori_loop(0, CHUNKS, mid, 0)

        def back(n, _):
            backward_unit(n // NSUB, n % NSUB, False)
            return 0

        lax.fori_loop(0, (CHUNKS - 1) * NSUB, back, 0)
        PS[...] = jnp.zeros((2, BAND, LON), F32)

        def back_last(u, _):
            backward_unit(CHUNKS - 1, u, True)
            return 0

        lax.fori_loop(0, NSUB, back_last, 0)
        stats_out()
        e_start()

        @pl.when(l == 0)
        def _():
            rs_start()
            rs_sum()
            RED[6] = TC[...]
            RED[5] = e_sum()
            ag_start(seven)
            ag_wait(seven)
            TC[...] = over_channels([AG[d, 6] for d in range(8)])
            EN[...] = over_channels([AG[d, 5] for d in range(8)])
            rs_sent()
            ag_sent(seven)

        @pl.when(l == 1)
        def _():
            RED[5] = e_sum()
            for a, b in CH_ORDER:
                af_copy(a, b).start()
            AF[mc] = RED[5]
            for a, b in CH_ORDER:
                af_from(a, b).wait_recv()
            EN[...] = over_channels([AF[d] for d in range(8)])
            for a, b in CH_ORDER:
                af_copy(a, b).wait_send()

        e_sent()

        def sent(n, _):
            c = n // NSUB
            u = n % NSUB
            unit_whole(SF, RF, fs, fr, c, u).wait_send()
            unit_whole(SB, RB, bs, br, c, u).wait_send()
            return 0

        lax.fori_loop(0, CHUNKS * NSUB, sent, 0)
        return jnp.sqrt(TC[...] / EN[...])

    scale = lax.fori_loop(0, 2, layer, jnp.ones((8, 128), F32))
    srow = scale[0:1, 0:1]

    def finish(i, _):
        rows = pl.ds(pl.multiple_of(i * 96, 96), 96)
        o_ref[rows, :] = (V[rows, :] * srow).astype(BF16)
        return 0

    lax.fori_loop(0, ROWS // 96, finish, 0)


def per_device(field_in, ln_gain, ln_shift, mix_first, mix_bias, mix_second):
    vm = pl.BlockSpec(memory_space=pltpu.VMEM)
    sm = pl.BlockSpec(memory_space=pltpu.SMEM)
    hbm = pl.BlockSpec(memory_space=pl.ANY)
    dma = pltpu.SemaphoreType.DMA
    buf = pltpu.VMEM((CHUNKS, NSUB, N_LAT, SUBROWS, 128), BF16)
    unit = dma((CHUNKS, NSUB))
    out = pl.pallas_call(
        kernel,
        out_shape=jax.ShapeDtypeStruct((ROWS, LON), BF16),
        in_specs=[hbm] * 3 + [vm] * 4 + [sm] * 2,
        out_specs=vm,
        scratch_shapes=[
            pltpu.VMEM((ROWS, LON), BF16),
            pltpu.VMEM((CHUNKS, 256, LON), BF16),
            pltpu.VMEM((2, LATS, LATS), BF16),
            pltpu.VMEM((ROWS, LON), F32),
            pltpu.VMEM((ROWS, LON), BF16),
            pltpu.VMEM((CHUNKS, LON, 256), BF16),
            pltpu.VMEM((CHUNKS, 256, LON), BF16),
            pltpu.VMEM((2 * LATS, 2 * LATS), BF16),
            pltpu.VMEM((2 * LATS, 2 * LATS), BF16),
            buf,
            buf,
            buf,
            buf,
            pltpu.VMEM((16, CHN, LATS), F32),
            pltpu.VMEM((384, 256), F32),
            pltpu.VMEM((384, 2 * LATS), BF16),
            pltpu.VMEM((384, 2 * LATS), BF16),
            pltpu.VMEM((256, 256), F32),
            pltpu.VMEM((2, 192, 192), BF16),
            pltpu.VMEM((2, 192, 192), BF16),
            pltpu.VMEM((128, 128), F32),
            pltpu.VMEM((2, 192, 128), F32),
            pltpu.VMEM((2, BAND, LON), F32),
            pltpu.VMEM((40, 8, 128), F32),
            pltpu.VMEM((8, 5, 8, 128), F32),
            pltpu.VMEM((7, 8, 128), F32),
            pltpu.VMEM((8, 7, 8, 128), F32),
            pltpu.VMEM((8, 8, 128), F32),
            pltpu.VMEM((8, 128), F32),
            pltpu.VMEM((N_LAT, 8, 128), F32),
            pltpu.VMEM((8, 128), F32),
            pltpu.VMEM((8, 128), F32),
            pltpu.VMEM((2, BAND, LON), F32),
            dma((6,)),
            dma((2,)),
            unit,
            unit,
            unit,
            unit,
            dma((8,)),
            dma((8,)),
            dma((8,)),
            dma((8,)),
            dma((8,)),
            dma((8,)),
            dma((N_LAT,)),
            dma((N_LAT,)),
        ],
        compiler_params=pltpu.CompilerParams(
            collective_id=0, has_side_effects=True, vmem_limit_bytes=60 * 1024 * 1024
        ),
    )(
        field_in.reshape(ROWS, LON), lon_table(), lat_tables(), mix_first[:, :, 0], mix_bias[:, :, 0],
        mix_second[:, :, 0], area_table(), ln_gain, ln_shift,
    )
    return out.reshape(CHN, BAND, LON)


def solution(mesh):
    finer = Mesh(mesh.devices.reshape(4, 4, 4, 2), ("lat_0", "lat_1", "ch_0", "ch_1"))
    in_specs = (
        P(CH, LAT, None),
        P(None, CH),
        P(None, CH),
        P(None, None, CH, None, None),
        P(None, None, CH, None),
        P(None, None, CH, None, None),
    )
    return jax.shard_map(
        per_device, mesh=finer, in_specs=in_specs, out_specs=P(CH, LAT, None), check_vma=False
    )
```

```python
import math

import jax
import jax.numpy as jnp
import numpy as np
from jax import lax
from jax.experimental import pallas as pl
from jax.experimental.pallas import tpu as pltpu
from jax.sharding import Mesh
from jax.sharding import PartitionSpec as P

CH = ("ch_0", "ch_1")
LAT = ("lat_0", "lat_1")
MESH = pl.DeviceIdType.MESH

norm_eps = 1e-05
shrink_level = 0.01

F32 = jnp.float32
BF16 = jnp.bfloat16

N_LAT = 16
BAND = 24
CHN = 96
ROWS = CHN * BAND
LON = 768
LATS = N_LAT * BAND
CHUNKS = 3
KL = 8
ALL_CH = 768
PIECE = 12 * BAND

ORDER = [
    (2, 2), (1, 2), (2, 1), (2, 3), (3, 2), (0, 2), (1, 1), (1, 3), (2, 0),
    (3, 1), (3, 3), (0, 1), (0, 3), (1, 0), (3, 0),
]
CH_ORDER = [(1, 0), (3, 0), (1, 1), (3, 1), (2, 0), (2, 1), (0, 1)]


NSUB = 6
SUBSTEPS = 6 // NSUB
SUBROWS = PIECE // NSUB


def trig(length, n, f):
    ang = (n * f % length) * (2.0 * math.pi / length)
    scale = 1.0 / math.sqrt(length)
    return np.cos(ang) * scale, np.sin(ang) * scale


def lon_table():
    row = np.arange(LON)
    kk = row // 8 % 16
    q = row // 128 % 2 * 8 + row % 8
    mode = q * BAND + row // 256 * KL + kk % KL
    cs, sn = trig(LON, mode[:, None], np.arange(LON)[None, :])
    return np.where((kk < KL)[:, None], cs, -sn).reshape(CHUNKS, 256, LON).astype(BF16)


def lat_tables():
    n = np.arange(LATS)
    cs, sn = trig(LATS, n[:, None], n[None, :])
    return np.stack([cs, sn]).astype(BF16)


def area_table():
    row = np.arange(LATS, dtype=np.float32).reshape(N_LAT, BAND, 1)
    area = np.cos((row + 0.5) * (math.pi / LATS) - 0.5 * math.pi)
    return np.broadcast_to(area, (N_LAT, BAND, 128)).astype(np.float32)


def kernel(
    x_hbm, tb_hbm, cs_hbm, w1_hbm, b_hbm, w2_hbm, area_hbm, gain_hbm, shift_hbm,
    o_hbm, SC,
    X, TB, CS, w1_ref, b_ref, w2_ref, area_ref, gain_ref, shift_ref, V, N, TF, TI, LF, LI, SF, RF, SB, RB, G, R, SP, MX, AW, A1, A2, BT, B1,
    PS, ST, RS, RED, AG, EX, AE, AT, AF, ES, EB, TC, EN, MI,
    xs, ts, os, fs, fr, bs, br, rss, rsr, ags, agr, aes, aer, ats, atr, afs, afr, es, er,
):
    y = lax.axis_index("lat_0")
    z = lax.axis_index("lat_1")
    cx = lax.axis_index("ch_0")
    ck = lax.axis_index("ch_1")
    me = y * 4 + z
    mc = cx * 2 + ck

    def x_copy(i):
        rows = pl.ds(pl.multiple_of(i * 384, 384), 384)
        return pltpu.make_async_copy(x_hbm.at[rows], X.at[rows], xs.at[i])

    for i in range(6):
        x_copy(i).start()
    small = [
        pltpu.make_async_copy(src, dst, ts.at[n])
        for n, (src, dst) in enumerate(
            (
                (area_hbm.at[me], area_ref),
                (tb_hbm, TB),
                (cs_hbm, CS),
                (w1_hbm, w1_ref),
                (b_hbm, b_ref),
                (w2_hbm, w2_ref),
                (gain_hbm, gain_ref),
                (shift_hbm, shift_ref),
            )
        )
    ]
    for copy in small:
        copy.start()

    def lat_to(a, b):
        yy = lax.rem(y + a, 4)
        zz = lax.rem(z + b, 4)
        return {"lat_0": yy, "lat_1": zz}, yy * 4 + zz

    def ch_to(a, b):
        xx = lax.rem(cx + a, 4)
        kk = lax.rem(ck + b, 2)
        return {"ch_0": xx, "ch_1": kk}, xx * 2 + kk

    bar = pltpu.get_barrier_semaphore()
    for a, b in ORDER:
        pl.semaphore_signal(bar, 1, device_id=lat_to(a, b)[0], device_id_type=MESH)
    for a, b in CH_ORDER:
        pl.semaphore_signal(bar, 1, device_id=ch_to(a, b)[0], device_id_type=MESH)

    def rcopy(src, dst, ss, rr, dev):
        return pltpu.make_async_remote_copy(
            src_ref=src, dst_ref=dst, send_sem=ss, recv_sem=rr, device_id=dev, device_id_type=MESH
        )

    def unit_start(sb, rb, ss, rr, c, u):
        for a, b in ORDER:
            dev, q = lat_to(a, b)
            rcopy(sb.at[c, u, q], rb.at[c, u, me], ss.at[c, u], rr.at[c, u], dev).start()
        rb[c, u, me] = sb[c, u, me]

    def unit_whole(sb, rb, ss, rr, c, u):
        peers = pl.ds(0, N_LAT - 1)
        dev = lat_to(1, 0)[0]
        return rcopy(sb.at[c, u, peers], rb.at[c, u, peers], ss.at[c, u], rr.at[c, u], dev)

    def stats_out():
        e = jnp.zeros((8, 128), F32)
        for hb in range(3):
            for lb in range(6):
                t = hb * 6 + lb
                rows, lanes = slice(8 * hb, 8 * hb + 8), slice(128 * lb, 128 * lb + 128)
                sq = PS[1, rows, lanes]
                ST[t] = PS[0, rows, lanes]
                ST[18 + t] = sq
                e = e + sq * area_ref[rows, :]
        ES[...] = jnp.sum(e, axis=0, keepdims=True)

    def e_copy(a, b):
        dev, q = lat_to(a, b)
        return rcopy(ES, EB.at[me], es.at[q], er.at[me], dev)

    def e_from(a, b):
        dev, p = lat_to(4 - a, 4 - b)
        return rcopy(ES, EB.at[p], es.at[p], er.at[p], dev)

    def rs_copy(a, b):
        dev, d = ch_to(a, b)
        return rcopy(ST.at[pl.ds(5 * d, 5)], RS.at[mc], rss.at[d], rsr.at[mc], dev)

    def rs_from(a, b):
        dev, d = ch_to(4 - a, 2 - b)
        return rcopy(ST.at[pl.ds(5 * d, 5)], RS.at[d], rss.at[d], rsr.at[d], dev)

    def ag_copy(a, b):
        dev, d = ch_to(a, b)
        return rcopy(RED, AG.at[mc], ags.at[d], agr.at[mc], dev)

    def ag_from(a, b):
        dev, d = ch_to(4 - a, 2 - b)
        return rcopy(RED, AG.at[d], ags.at[d], agr.at[d], dev)

    def rs_start():
        for a, b in CH_ORDER:
            rs_copy(a, b).start()
        RS[mc] = ST[pl.ds(5 * mc, 5)]

    def e_start():
        for a, b in ORDER:
            e_copy(a, b).start()
        EB[me] = ES[...]

    def rs_sum():
        for a, b in CH_ORDER:
            rs_from(a, b).wait_recv()
        tot = RS[0]
        for d in range(1, 8):
            tot = tot + RS[d]
        RED[...] = tot

    def e_sum():
        for a, b in ORDER:
            e_from(a, b).wait_recv()
        e = EB[0]
        for p in range(1, N_LAT):
            e = e + EB[p]
        return e

    def ag_start():
        for a, b in CH_ORDER:
            ag_copy(a, b).start()
        AG[mc] = RED[...]

    def ag_wait():
        for a, b in CH_ORDER:
            ag_from(a, b).wait_recv()

    def rs_sent():
        for a, b in CH_ORDER:
            rs_copy(a, b).wait_send()

    def ag_sent():
        for a, b in CH_ORDER:
            ag_copy(a, b).wait_send()

    def e_sent():
        for a, b in ORDER:
            e_copy(a, b).wait_send()

    def row_copy(n, dst, ss, rr, a, b):
        dev, d = ch_to(a, b)
        return rcopy(EX.at[n], dst.at[mc], ss.at[d], rr.at[mc], dev)

    def row_from(n, dst, ss, rr, a, b):
        dev, d = ch_to(4 - a, 2 - b)
        return rcopy(EX.at[n], dst.at[d], ss.at[d], rr.at[d], dev)

    def row_start(n, dst, ss, rr):
        for a, b in CH_ORDER:
            row_copy(n, dst, ss, rr, a, b).start()
        dst[mc] = EX[n]

    def row_sum(n, dst, ss, rr):
        for a, b in CH_ORDER:
            row_from(n, dst, ss, rr, a, b).wait_recv()
        return over_channels([dst[d] for d in range(8)])

    def row_sent(n, dst, ss, rr):
        for a, b in CH_ORDER:
            row_copy(n, dst, ss, rr, a, b).wait_send()

    def over_channels(tiles):
        e = tiles[0]
        for d in range(1, 8):
            e = e + tiles[d]
        e = jnp.sum(e, axis=1, keepdims=True)
        return jnp.broadcast_to(e, (8, 128))

    def lane_masks():
        lane = lax.broadcasted_iota(jnp.int32, (48, 128), 1) & 7
        return [lane == s for s in range(8)]

    def block_swap(parts, masks):
        rolled = [p if r == 0 else pltpu.roll(p, r, 1) for r, p in enumerate(parts)]
        out = []
        for q in range(8):
            acc = rolled[-q % 8]
            for s in range(1, 8):
                acc = jnp.where(masks[s], rolled[(s - q) % 8], acc)
            out.append(acc if q == 0 else pltpu.roll(acc, 128 - q, 1))
        return out

    def rows_of(ii):
        return pl.ds(pl.multiple_of(ii * 48, 48), 48)

    def forward_step(c, u, ii):
        base = pl.multiple_of((u * SUBSTEPS + ii) * 384, 384)
        R[...] = jnp.dot(N[pl.ds(base, 384), :], TF[c], preferred_element_type=F32)
        masks = lane_masks()
        for half in range(2):
            hs = slice(128 * half, 128 * half + 128)
            parts = [
                jnp.concatenate(
                    [R[24 * r : 24 * r + 24, hs], R[192 + 24 * r : 216 + 24 * r, hs]], axis=0
                )
                for r in range(8)
            ]
            for q, piece in enumerate(block_swap(parts, masks)):
                SF[c, u, 8 * half + q, rows_of(ii), :] = piece.astype(BF16)

    def normalize_step(l, srow, i):
        def pair(j, _):
            base = i * 384 + j * 48
            ch = i * 16 + j * 2
            for lb in range(2):
                ls = slice(384 * lb, 384 * lb + 384)
                mean = MI[0, :, ls]
                inv = MI[1, :, ls]
                both = []
                for t in range(2):
                    rows = pl.ds(pl.multiple_of(base + 24 * t, 24), 24)
                    cur = (V[rows, ls] * srow).astype(BF16).astype(F32)
                    nrm = (cur - mean) * inv * gain_ref[l, ch + t] + shift_ref[l, ch + t]
                    nrm = nrm.astype(BF16).astype(F32)
                    V[rows, ls] = cur + nrm
                    both.append(nrm)
                N[pl.ds(pl.multiple_of(base, 48), 48), ls] = jnp.concatenate(both, axis=0).astype(BF16)
            return 0

        lax.fori_loop(0, 8, pair, 0)

    def forward_first(l, srow):
        def unit(u, _):
            def step(ii, _):
                normalize_step(l, srow, u * SUBSTEPS + ii)
                forward_step(0, u, ii)
                return 0

            lax.fori_loop(0, SUBSTEPS, step, 0)
            unit_start(SF, RF, fs, fr, 0, u)
            return 0

        lax.fori_loop(0, NSUB, unit, 0)

    def forward_rest():
        def unit(n, _):
            c = n // NSUB
            u = n % NSUB

            def step(ii, _):
                forward_step(c, u, ii)
                return 0

            lax.fori_loop(0, SUBSTEPS, step, 0)
            unit_start(SF, RF, fs, fr, c, u)
            return 0

        lax.fori_loop(NSUB, CHUNKS * NSUB, unit, 0)

    def middle_chunk(l, c):
        def gather_unit(u, _):
            unit_whole(SF, RF, fs, fr, c, u).wait_recv()

            def gather(ii, _):
                i = u * SUBSTEPS + ii
                got = [RF[c, u, p, rows_of(ii), :].astype(F32) for p in range(N_LAT)]
                for j in range(2):
                    blk = jnp.concatenate([g[24 * j : 24 * j + 24] for g in got], axis=0)
                    t = blk.T.reshape(16, 8, LATS)
                    G[:, pl.ds(pl.multiple_of(i * 16 + 8 * j, 8), 8), :] = t
                return 0

            lax.fori_loop(0, SUBSTEPS, gather, 0)
            return 0

        lax.fori_loop(0, NSUB, gather_unit, 0)

        def mix(b, _):
            g_re = G[pl.ds(4 * b, 4)].reshape(384, LATS).astype(BF16)
            g_im = G[pl.ds(8 + 4 * b, 4)].reshape(384, LATS).astype(BF16)
            SP[...] = jnp.dot(
                jnp.concatenate([g_re, g_im], axis=1), LF[...], preferred_element_type=F32
            ).astype(BF16)
            bias = jnp.concatenate([B1[l]] * 3, axis=1)
            for k in range(4):
                rows = slice(96 * k, 96 * k + 96)
                both = jnp.concatenate([SP[rows, 0:LATS], SP[rows, LATS:]], axis=0)
                hid = jnp.dot(A1[l], both, preferred_element_type=F32) + bias
                hid = jnp.maximum(hid, 0.0).astype(BF16)
                m = jnp.dot(A2[l], hid, preferred_element_type=F32)
                m = (m - jnp.clip(m, -shrink_level, shrink_level)).astype(BF16)
                MX[rows, 0:LATS] = m[0:96]
                MX[rows, LATS:] = m[96:192]
            back = jnp.dot(MX[...], LI[...], preferred_element_type=F32)
            G[pl.ds(4 * b, 4)] = back[:, 0:LATS].reshape(4, CHN, LATS)
            G[pl.ds(8 + 4 * b, 4)] = back[:, LATS:].reshape(4, CHN, LATS)
            return 0

        lax.fori_loop(0, 2, mix, 0)

        def scatter_unit(u, _):
            def scatter(ii, _):
                i = u * SUBSTEPS + ii
                ts = []
                for j in range(2):
                    blk = G[:, pl.ds(pl.multiple_of(i * 16 + 8 * j, 8), 8), :].reshape(128, LATS)
                    ts.append(blk.T)
                for p in range(N_LAT):
                    piece = jnp.concatenate([t[24 * p : 24 * p + 24] for t in ts], axis=0)
                    SB[c, u, p, rows_of(ii), :] = piece.astype(BF16)
                return 0

            lax.fori_loop(0, SUBSTEPS, scatter, 0)
            unit_start(SB, RB, bs, br, c, u)
            return 0

        lax.fori_loop(0, NSUB, scatter_unit, 0)

    def o_copy(i):
        rows = pl.ds(pl.multiple_of(i * 384, 384), 384)
        return pltpu.make_async_copy(X.at[rows], o_hbm.at[rows], os.at[i])

    def backward_unit(l, c, u, last):
        unit_whole(SB, RB, bs, br, c, u).wait_recv()

        def step(ii, _):
            masks = lane_masks()
            for half in range(2):
                hs = slice(128 * half, 128 * half + 128)
                parts = [RB[c, u, 8 * half + q, rows_of(ii), :].astype(F32) for q in range(8)]
                for r, piece in enumerate(block_swap(parts, masks)):
                    R[24 * r : 24 * r + 24, hs] = piece[0:24]
                    R[192 + 24 * r : 216 + 24 * r, hs] = piece[24:48]
            rows = pl.ds(pl.multiple_of((u * SUBSTEPS + ii) * 384, 384), 384)
            v = V[rows, :] + jnp.dot(R[...].astype(BF16), TI[c], preferred_element_type=F32)
            V[rows, :] = v
            if last:
                X[rows, :] = v.astype(BF16)

                @pl.when(l == 1)
                def _():
                    o_copy(u * SUBSTEPS + ii).start()

                v = v.reshape(16, BAND, LON)
                PS[0] += jnp.sum(v, axis=0)
                PS[1] += jnp.sum(v * v, axis=0)
            return 0

        lax.fori_loop(0, SUBSTEPS, step, 0)

    def set_tables():
        for copy in small[1:]:
            copy.wait()
        row = lax.broadcasted_iota(jnp.int32, (256, LON), 0)
        for c in range(CHUNKS):
            t = TB[c].astype(F32)
            TF[c] = t.T.astype(BF16)
            twice = t * 2.0
            TI[c] = (jnp.where(row == 0, t, twice) if c == 0 else twice).astype(BF16)
        cl = CS[0]
        sl = CS[1]
        LF[0:LATS, 0:LATS] = cl
        LF[0:LATS, LATS:] = -sl
        LF[LATS:, 0:LATS] = sl
        LF[LATS:, LATS:] = cl
        LI[0:LATS, 0:LATS] = cl
        LI[0:LATS, LATS:] = sl
        LI[LATS:, 0:LATS] = -sl
        LI[LATS:, LATS:] = cl
        AW[...] = jnp.zeros((256, 256), F32)
        BT[...] = jnp.zeros((128, 128), F32)
        for l in range(2):
            for w_ref, a_ref in ((w1_ref, A1), (w2_ref, A2)):
                re = w_ref[l, 0].astype(F32)
                im = w_ref[l, 1].astype(F32)
                AW[0:96, 0:192] = jnp.concatenate([re, im], axis=1)
                AW[96:192, 0:192] = jnp.concatenate([-im, re], axis=1)
                a_ref[l] = AW[...].T[0:192, 0:192].astype(BF16)
            for part in range(2):
                BT[:, 0:96] = jnp.broadcast_to(b_ref[l, part : part + 1, :].astype(F32), (128, 96))
                B1[l, 96 * part : 96 * part + 96, :] = BT[...].T[0:96, :]

    def set_mean_inv(scale):
        for hb in range(3):
            for lb in range(6):
                t = hb * 6 + lb
                u = t + 18
                mean = AG[t // 5, t % 5] * scale * (1.0 / ALL_CH)
                spread = AG[u // 5, u % 5] * (scale * scale) * (1.0 / ALL_CH) - mean * mean
                MI[0, 8 * hb : 8 * hb + 8, 128 * lb : 128 * lb + 128] = mean
                MI[1, 8 * hb : 8 * hb + 8, 128 * lb : 128 * lb + 128] = lax.rsqrt(spread + norm_eps)

    by_energy = (0, AE, aes, aer)
    by_target = (1, AT, ats, atr)
    by_last = (0, AF, afs, afr)

    zero = jnp.zeros((BAND, LON), F32)
    for t in range(36, 40):
        ST[t] = jnp.zeros((8, 128), F32)

    def first_block(i, carry):
        x_copy(i).wait()

        def pair(j, carry):
            s1, s2 = carry
            rows = pl.ds(pl.multiple_of(i * 384 + j * 48, 48), 48)
            xx = X[rows, :].astype(F32)
            V[rows, :] = xx
            for t in range(2):
                v = xx[24 * t : 24 * t + 24]
                s1 = s1 + v
                s2 = s2 + v * v
            return s1, s2

        return lax.fori_loop(0, 8, pair, carry)

    s1, s2 = lax.fori_loop(0, 6, first_block, (zero, zero))
    PS[0] = s1
    PS[1] = s2
    small[0].wait()
    stats_out()
    pl.semaphore_wait(bar, len(ORDER) + len(CH_ORDER))
    rs_start()
    e_start()
    set_tables()
    rs_sum()
    ag_start()
    EX[1] = e_sum()
    ag_wait()
    rs_sent()
    ag_sent()
    e_sent()

    def layer(l, scale):
        set_mean_inv(scale)
        srow = scale[0:1, 0:1]
        forward_first(l, srow)
        forward_rest()

        def mid(c, _):
            middle_chunk(l, c)
            return 0

        lax.fori_loop(0, CHUNKS, mid, 0)

        def back(n, _):
            backward_unit(l, n // NSUB, n % NSUB, False)
            return 0

        lax.fori_loop(0, (CHUNKS - 1) * NSUB, back, 0)
        PS[...] = jnp.zeros((2, BAND, LON), F32)

        def back_last(u, _):
            backward_unit(l, CHUNKS - 1, u, True)
            return 0

        lax.fori_loop(0, NSUB, back_last, 0)
        stats_out()

        @pl.when(l == 0)
        def _():
            rs_start()
            e_start()
            row_start(*by_target)
            rs_sum()
            ag_start()
            EX[0] = e_sum()
            row_start(*by_energy)
            TC[...] = row_sum(*by_target)
            ag_wait()
            EN[...] = row_sum(*by_energy)
            rs_sent()
            ag_sent()
            row_sent(*by_target)
            row_sent(*by_energy)

        @pl.when(l == 1)
        def _():
            e_start()
            EX[0] = e_sum()
            row_start(*by_last)
            EN[...] = row_sum(*by_last)
            row_sent(*by_last)

        e_sent()

        def sent(n, _):
            c = n // NSUB
            u = n % NSUB
            unit_whole(SF, RF, fs, fr, c, u).wait_send()
            unit_whole(SB, RB, bs, br, c, u).wait_send()
            return 0

        lax.fori_loop(0, CHUNKS * NSUB, sent, 0)
        return jnp.sqrt(TC[...] / EN[...])

    scale = lax.fori_loop(0, 2, layer, jnp.ones((8, 128), F32))
    SC[...] = scale
    for i in range(6):
        o_copy(i).wait()


def scale_kernel(v_hbm, s_hbm, o_hbm, vin, sin, vout, si, so, ss):
    def rows(n):
        return slice(192 * n, 192 * n + 192)

    def come(n):
        return pltpu.make_async_copy(v_hbm.at[rows(n)], vin.at[rows(n)], si.at[n])

    def go(n):
        return pltpu.make_async_copy(vout.at[rows(n)], o_hbm.at[rows(n)], so.at[n])

    get_scale = pltpu.make_async_copy(s_hbm, sin, ss)
    get_scale.start()
    for n in range(12):
        come(n).start()
    get_scale.wait()
    scale = sin[0:1, 0:1]
    for n in range(12):
        come(n).wait()
        vout[rows(n), :] = (vin[rows(n), :].astype(F32) * scale).astype(BF16)
        go(n).start()
    for n in range(12):
        go(n).wait()


def per_device(field_in, ln_gain, ln_shift, mix_first, mix_bias, mix_second):
    vm = pl.BlockSpec(memory_space=pltpu.VMEM)
    hbm = pl.BlockSpec(memory_space=pl.ANY)
    dma = pltpu.SemaphoreType.DMA
    buf = pltpu.VMEM((CHUNKS, NSUB, N_LAT, SUBROWS, 128), BF16)
    unit = dma((CHUNKS, NSUB))
    summed, scale = pl.pallas_call(
        kernel,
        out_shape=(
            jax.ShapeDtypeStruct((ROWS, LON), BF16),
            jax.ShapeDtypeStruct((8, 128), F32),
        ),
        in_specs=[hbm] * 9,
        out_specs=(hbm, vm),
        scratch_shapes=[
            pltpu.VMEM((ROWS, LON), BF16),
            pltpu.VMEM((CHUNKS, 256, LON), BF16),
            pltpu.VMEM((2, LATS, LATS), BF16),
            pltpu.VMEM((2, 2, CHN, CHN), BF16),
            pltpu.VMEM((2, 2, CHN), BF16),
            pltpu.VMEM((2, 2, CHN, CHN), BF16),
            pltpu.VMEM((BAND, 128), F32),
            pltpu.SMEM((2, CHN), F32),
            pltpu.SMEM((2, CHN), F32),
            pltpu.VMEM((ROWS, LON), F32),
            pltpu.VMEM((ROWS, LON), BF16),
            pltpu.VMEM((CHUNKS, LON, 256), BF16),
            pltpu.VMEM((CHUNKS, 256, LON), BF16),
            pltpu.VMEM((2 * LATS, 2 * LATS), BF16),
            pltpu.VMEM((2 * LATS, 2 * LATS), BF16),
            buf,
            buf,
            buf,
            buf,
            pltpu.VMEM((16, CHN, LATS), F32),
            pltpu.VMEM((384, 256), F32),
            pltpu.VMEM((384, 2 * LATS), BF16),
            pltpu.VMEM((384, 2 * LATS), BF16),
            pltpu.VMEM((256, 256), F32),
            pltpu.VMEM((2, 192, 192), BF16),
            pltpu.VMEM((2, 192, 192), BF16),
            pltpu.VMEM((128, 128), F32),
            pltpu.VMEM((2, 192, 128), F32),
            pltpu.VMEM((2, BAND, LON), F32),
            pltpu.VMEM((40, 8, 128), F32),
            pltpu.VMEM((8, 5, 8, 128), F32),
            pltpu.VMEM((5, 8, 128), F32),
            pltpu.VMEM((8, 5, 8, 128), F32),
            pltpu.VMEM((2, 1, 128), F32),
            pltpu.VMEM((8, 1, 128), F32),
            pltpu.VMEM((8, 1, 128), F32),
            pltpu.VMEM((8, 1, 128), F32),
            pltpu.VMEM((1, 128), F32),
            pltpu.VMEM((N_LAT, 1, 128), F32),
            pltpu.VMEM((8, 128), F32),
            pltpu.VMEM((8, 128), F32),
            pltpu.VMEM((2, BAND, LON), F32),
            dma((6,)),
            dma((8,)),
            dma((6,)),
            unit,
            unit,
            unit,
            unit,
            dma((8,)),
            dma((8,)),
            dma((8,)),
            dma((8,)),
            dma((8,)),
            dma((8,)),
            dma((8,)),
            dma((8,)),
            dma((8,)),
            dma((8,)),
            dma((N_LAT,)),
            dma((N_LAT,)),
        ],
        compiler_params=pltpu.CompilerParams(
            collective_id=0, has_side_effects=True, vmem_limit_bytes=60 * 1024 * 1024
        ),
    )(
        field_in.reshape(ROWS, LON), lon_table(), lat_tables(), mix_first[:, :, 0], mix_bias[:, :, 0],
        mix_second[:, :, 0], area_table(), ln_gain, ln_shift,
    )
    out = pl.pallas_call(
        scale_kernel,
        out_shape=jax.ShapeDtypeStruct((ROWS, LON), BF16),
        in_specs=[hbm, hbm],
        out_specs=hbm,
        scratch_shapes=[
            pltpu.VMEM((ROWS, LON), BF16),
            pltpu.VMEM((8, 128), F32),
            pltpu.VMEM((ROWS, LON), BF16),
            dma((12,)),
            dma((12,)),
            dma(()),
        ],
    )(summed, scale)
    return out.reshape(CHN, BAND, LON)


def solution(mesh):
    finer = Mesh(mesh.devices.reshape(4, 4, 4, 2), ("lat_0", "lat_1", "ch_0", "ch_1"))
    in_specs = (
        P(CH, LAT, None),
        P(None, CH),
        P(None, CH),
        P(None, None, CH, None, None),
        P(None, None, CH, None),
        P(None, None, CH, None, None),
    )
    return jax.shard_map(
        per_device, mesh=finer, in_specs=in_specs, out_specs=P(CH, LAT, None), check_vma=False
    )
```

```python
import math

import jax
import jax.numpy as jnp
import numpy as np
from jax import lax
from jax.experimental import pallas as pl
from jax.experimental.pallas import tpu as pltpu
from jax.sharding import Mesh
from jax.sharding import PartitionSpec as P

CH = ("ch_0", "ch_1")
LAT = ("lat_0", "lat_1")
MESH = pl.DeviceIdType.MESH

norm_eps = 1e-05
shrink_level = 0.01

F32 = jnp.float32
BF16 = jnp.bfloat16

N_LAT = 16
BAND = 24
CHN = 96
ROWS = CHN * BAND
LON = 768
LATS = N_LAT * BAND
CHUNKS = 3
KL = 8
ALL_CH = 768
PIECE = 12 * BAND

ORDER = [
    (2, 2), (1, 2), (2, 1), (2, 3), (3, 2), (0, 2), (1, 1), (1, 3), (2, 0),
    (3, 1), (3, 3), (0, 1), (0, 3), (1, 0), (3, 0),
]
CH_ORDER = [(1, 0), (3, 0), (1, 1), (3, 1), (2, 0), (2, 1), (0, 1)]


NSUB = 6
SUBSTEPS = 6 // NSUB
SUBROWS = PIECE // NSUB


def trig(length, n, f):
    ang = (n * f % length) * (2.0 * math.pi / length)
    scale = 1.0 / math.sqrt(length)
    return np.cos(ang) * scale, np.sin(ang) * scale


def lon_table():
    row = np.arange(LON)
    kk = row // 8 % 16
    q = row // 128 % 2 * 8 + row % 8
    mode = q * BAND + row // 256 * KL + kk % KL
    cs, sn = trig(LON, mode[:, None], np.arange(LON)[None, :])
    return np.where((kk < KL)[:, None], cs, -sn).reshape(CHUNKS, 256, LON).astype(BF16)


def lat_tables():
    n = np.arange(LATS)
    cs, sn = trig(LATS, n[:, None], n[None, :])
    return np.stack([cs, sn]).astype(BF16)


def area_table():
    row = np.arange(LATS, dtype=np.float32).reshape(N_LAT, BAND, 1)
    area = np.cos((row + 0.5) * (math.pi / LATS) - 0.5 * math.pi)
    return np.broadcast_to(area, (N_LAT, BAND, 128)).astype(np.float32)


def kernel(
    x_hbm, tb_hbm, cs_hbm, w1_hbm, b_hbm, w2_hbm, area_hbm, gain_hbm, shift_hbm,
    V, SC,
    X, TB, CS, w1_ref, b_ref, w2_ref, area_ref, gain_ref, shift_ref, N, TF, TI, LF, LI, SF, RF, SB, RB, G, R, SP, MX, AW, A1, A2, BT, B1,
    PS, ST, RS, RED, AG, EX, AE, AT, AF, ES, EB, TC, EN, MI,
    xs, ts, fs, fr, bs, br, rss, rsr, ags, agr, aes, aer, ats, atr, afs, afr, es, er,
):
    y = lax.axis_index("lat_0")
    z = lax.axis_index("lat_1")
    cx = lax.axis_index("ch_0")
    ck = lax.axis_index("ch_1")
    me = y * 4 + z
    mc = cx * 2 + ck

    def x_copy(i):
        rows = pl.ds(pl.multiple_of(i * 384, 384), 384)
        return pltpu.make_async_copy(x_hbm.at[rows], X.at[rows], xs.at[i])

    for i in range(6):
        x_copy(i).start()
    small = [
        pltpu.make_async_copy(src, dst, ts.at[n])
        for n, (src, dst) in enumerate(
            (
                (area_hbm.at[me], area_ref),
                (tb_hbm, TB),
                (cs_hbm, CS),
                (w1_hbm, w1_ref),
                (b_hbm, b_ref),
                (w2_hbm, w2_ref),
                (gain_hbm, gain_ref),
                (shift_hbm, shift_ref),
            )
        )
    ]
    for copy in small:
        copy.start()

    def lat_to(a, b):
        yy = lax.rem(y + a, 4)
        zz = lax.rem(z + b, 4)
        return {"lat_0": yy, "lat_1": zz}, yy * 4 + zz

    def ch_to(a, b):
        xx = lax.rem(cx + a, 4)
        kk = lax.rem(ck + b, 2)
        return {"ch_0": xx, "ch_1": kk}, xx * 2 + kk

    bar = pltpu.get_barrier_semaphore()
    for a, b in ORDER:
        pl.semaphore_signal(bar, 1, device_id=lat_to(a, b)[0], device_id_type=MESH)
    for a, b in CH_ORDER:
        pl.semaphore_signal(bar, 1, device_id=ch_to(a, b)[0], device_id_type=MESH)

    def rcopy(src, dst, ss, rr, dev):
        return pltpu.make_async_remote_copy(
            src_ref=src, dst_ref=dst, send_sem=ss, recv_sem=rr, device_id=dev, device_id_type=MESH
        )

    def unit_start(sb, rb, ss, rr, c, u):
        for a, b in ORDER:
            dev, q = lat_to(a, b)
            rcopy(sb.at[c, u, q], rb.at[c, u, me], ss.at[c, u], rr.at[c, u], dev).start()
        rb[c, u, me] = sb[c, u, me]

    def unit_whole(sb, rb, ss, rr, c, u):
        peers = pl.ds(0, N_LAT - 1)
        dev = lat_to(1, 0)[0]
        return rcopy(sb.at[c, u, peers], rb.at[c, u, peers], ss.at[c, u], rr.at[c, u], dev)

    def stats_out():
        e = jnp.zeros((8, 128), F32)
        for hb in range(3):
            for lb in range(6):
                t = hb * 6 + lb
                rows, lanes = slice(8 * hb, 8 * hb + 8), slice(128 * lb, 128 * lb + 128)
                sq = PS[1, rows, lanes]
                ST[t] = PS[0, rows, lanes]
                ST[18 + t] = sq
                e = e + sq * area_ref[rows, :]
        ES[...] = jnp.sum(e, axis=0, keepdims=True)

    def e_copy(a, b):
        dev, q = lat_to(a, b)
        return rcopy(ES, EB.at[me], es.at[q], er.at[me], dev)

    def e_from(a, b):
        dev, p = lat_to(4 - a, 4 - b)
        return rcopy(ES, EB.at[p], es.at[p], er.at[p], dev)

    def rs_copy(a, b):
        dev, d = ch_to(a, b)
        return rcopy(ST.at[pl.ds(5 * d, 5)], RS.at[mc], rss.at[d], rsr.at[mc], dev)

    def rs_from(a, b):
        dev, d = ch_to(4 - a, 2 - b)
        return rcopy(ST.at[pl.ds(5 * d, 5)], RS.at[d], rss.at[d], rsr.at[d], dev)

    def ag_copy(a, b):
        dev, d = ch_to(a, b)
        return rcopy(RED, AG.at[mc], ags.at[d], agr.at[mc], dev)

    def ag_from(a, b):
        dev, d = ch_to(4 - a, 2 - b)
        return rcopy(RED, AG.at[d], ags.at[d], agr.at[d], dev)

    def rs_start():
        for a, b in CH_ORDER:
            rs_copy(a, b).start()
        RS[mc] = ST[pl.ds(5 * mc, 5)]

    def e_start():
        for a, b in ORDER:
            e_copy(a, b).start()
        EB[me] = ES[...]

    def rs_sum():
        for a, b in CH_ORDER:
            rs_from(a, b).wait_recv()
        tot = RS[0]
        for d in range(1, 8):
            tot = tot + RS[d]
        RED[...] = tot

    def e_sum():
        for a, b in ORDER:
            e_from(a, b).wait_recv()
        e = EB[0]
        for p in range(1, N_LAT):
            e = e + EB[p]
        return e

    def ag_start():
        for a, b in CH_ORDER:
            ag_copy(a, b).start()
        AG[mc] = RED[...]

    def ag_wait():
        for a, b in CH_ORDER:
            ag_from(a, b).wait_recv()

    def rs_sent():
        for a, b in CH_ORDER:
            rs_copy(a, b).wait_send()

    def ag_sent():
        for a, b in CH_ORDER:
            ag_copy(a, b).wait_send()

    def e_sent():
        for a, b in ORDER:
            e_copy(a, b).wait_send()

    def row_copy(n, dst, ss, rr, a, b):
        dev, d = ch_to(a, b)
        return rcopy(EX.at[n], dst.at[mc], ss.at[d], rr.at[mc], dev)

    def row_from(n, dst, ss, rr, a, b):
        dev, d = ch_to(4 - a, 2 - b)
        return rcopy(EX.at[n], dst.at[d], ss.at[d], rr.at[d], dev)

    def row_start(n, dst, ss, rr):
        for a, b in CH_ORDER:
            row_copy(n, dst, ss, rr, a, b).start()
        dst[mc] = EX[n]

    def row_sum(n, dst, ss, rr):
        for a, b in CH_ORDER:
            row_from(n, dst, ss, rr, a, b).wait_recv()
        return over_channels([dst[d] for d in range(8)])

    def row_sent(n, dst, ss, rr):
        for a, b in CH_ORDER:
            row_copy(n, dst, ss, rr, a, b).wait_send()

    def over_channels(tiles):
        e = tiles[0]
        for d in range(1, 8):
            e = e + tiles[d]
        e = jnp.sum(e, axis=1, keepdims=True)
        return jnp.broadcast_to(e, (8, 128))

    def lane_masks():
        lane = lax.broadcasted_iota(jnp.int32, (48, 128), 1) & 7
        return [lane == s for s in range(8)]

    def block_swap(parts, masks):
        rolled = [p if r == 0 else pltpu.roll(p, r, 1) for r, p in enumerate(parts)]
        out = []
        for q in range(8):
            acc = rolled[-q % 8]
            for s in range(1, 8):
                acc = jnp.where(masks[s], rolled[(s - q) % 8], acc)
            out.append(acc if q == 0 else pltpu.roll(acc, 128 - q, 1))
        return out

    def rows_of(ii):
        return pl.ds(pl.multiple_of(ii * 48, 48), 48)

    def forward_step(c, u, ii):
        base = pl.multiple_of((u * SUBSTEPS + ii) * 384, 384)
        R[...] = jnp.dot(N[pl.ds(base, 384), :], TF[c], preferred_element_type=F32)
        masks = lane_masks()
        for half in range(2):
            hs = slice(128 * half, 128 * half + 128)
            parts = [
                jnp.concatenate(
                    [R[24 * r : 24 * r + 24, hs], R[192 + 24 * r : 216 + 24 * r, hs]], axis=0
                )
                for r in range(8)
            ]
            for q, piece in enumerate(block_swap(parts, masks)):
                SF[c, u, 8 * half + q, rows_of(ii), :] = piece.astype(BF16)

    def normalize_step(l, srow, i):
        def pair(j, _):
            base = i * 384 + j * 48
            ch = i * 16 + j * 2
            for lb in range(2):
                ls = slice(384 * lb, 384 * lb + 384)
                mean = MI[0, :, ls]
                inv = MI[1, :, ls]
                both = []
                for t in range(2):
                    rows = pl.ds(pl.multiple_of(base + 24 * t, 24), 24)
                    cur = (V[rows, ls] * srow).astype(BF16).astype(F32)
                    nrm = (cur - mean) * inv * gain_ref[l, ch + t] + shift_ref[l, ch + t]
                    nrm = nrm.astype(BF16).astype(F32)
                    V[rows, ls] = cur + nrm
                    both.append(nrm)
                N[pl.ds(pl.multiple_of(base, 48), 48), ls] = jnp.concatenate(both, axis=0).astype(BF16)
            return 0

        lax.fori_loop(0, 8, pair, 0)

    def forward_first(l, srow):
        def unit(u, _):
            def step(ii, _):
                normalize_step(l, srow, u * SUBSTEPS + ii)
                forward_step(0, u, ii)
                return 0

            lax.fori_loop(0, SUBSTEPS, step, 0)
            unit_start(SF, RF, fs, fr, 0, u)
            return 0

        lax.fori_loop(0, NSUB, unit, 0)

    def forward_rest():
        def unit(n, _):
            c = n // NSUB
            u = n % NSUB

            def step(ii, _):
                forward_step(c, u, ii)
                return 0

            lax.fori_loop(0, SUBSTEPS, step, 0)
            unit_start(SF, RF, fs, fr, c, u)
            return 0

        lax.fori_loop(NSUB, CHUNKS * NSUB, unit, 0)

    def middle_chunk(l, c):
        def gather_unit(u, _):
            unit_whole(SF, RF, fs, fr, c, u).wait_recv()

            def gather(ii, _):
                i = u * SUBSTEPS + ii
                got = [RF[c, u, p, rows_of(ii), :].astype(F32) for p in range(N_LAT)]
                for j in range(2):
                    blk = jnp.concatenate([g[24 * j : 24 * j + 24] for g in got], axis=0)
                    t = blk.T.reshape(16, 8, LATS)
                    G[:, pl.ds(pl.multiple_of(i * 16 + 8 * j, 8), 8), :] = t
                return 0

            lax.fori_loop(0, SUBSTEPS, gather, 0)
            return 0

        lax.fori_loop(0, NSUB, gather_unit, 0)

        def mix(b, _):
            g_re = G[pl.ds(4 * b, 4)].reshape(384, LATS).astype(BF16)
            g_im = G[pl.ds(8 + 4 * b, 4)].reshape(384, LATS).astype(BF16)
            SP[...] = jnp.dot(
                jnp.concatenate([g_re, g_im], axis=1), LF[...], preferred_element_type=F32
            ).astype(BF16)
            bias = jnp.concatenate([B1[l]] * 3, axis=1)
            for k in range(4):
                rows = slice(96 * k, 96 * k + 96)
                both = jnp.concatenate([SP[rows, 0:LATS], SP[rows, LATS:]], axis=0)
                hid = jnp.dot(A1[l], both, preferred_element_type=F32) + bias
                hid = jnp.maximum(hid, 0.0).astype(BF16)
                m = jnp.dot(A2[l], hid, preferred_element_type=F32)
                m = (m - jnp.clip(m, -shrink_level, shrink_level)).astype(BF16)
                MX[rows, 0:LATS] = m[0:96]
                MX[rows, LATS:] = m[96:192]
            back = jnp.dot(MX[...], LI[...], preferred_element_type=F32)
            G[pl.ds(4 * b, 4)] = back[:, 0:LATS].reshape(4, CHN, LATS)
            G[pl.ds(8 + 4 * b, 4)] = back[:, LATS:].reshape(4, CHN, LATS)
            return 0

        lax.fori_loop(0, 2, mix, 0)

        def scatter_unit(u, _):
            def scatter(ii, _):
                i = u * SUBSTEPS + ii
                ts = []
                for j in range(2):
                    blk = G[:, pl.ds(pl.multiple_of(i * 16 + 8 * j, 8), 8), :].reshape(128, LATS)
                    ts.append(blk.T)
                for p in range(N_LAT):
                    piece = jnp.concatenate([t[24 * p : 24 * p + 24] for t in ts], axis=0)
                    SB[c, u, p, rows_of(ii), :] = piece.astype(BF16)
                return 0

            lax.fori_loop(0, SUBSTEPS, scatter, 0)
            unit_start(SB, RB, bs, br, c, u)
            return 0

        lax.fori_loop(0, NSUB, scatter_unit, 0)

    def backward_unit(l, c, u, last):
        unit_whole(SB, RB, bs, br, c, u).wait_recv()

        def step(ii, _):
            masks = lane_masks()
            for half in range(2):
                hs = slice(128 * half, 128 * half + 128)
                parts = [RB[c, u, 8 * half + q, rows_of(ii), :].astype(F32) for q in range(8)]
                for r, piece in enumerate(block_swap(parts, masks)):
                    R[24 * r : 24 * r + 24, hs] = piece[0:24]
                    R[192 + 24 * r : 216 + 24 * r, hs] = piece[24:48]
            rows = pl.ds(pl.multiple_of((u * SUBSTEPS + ii) * 384, 384), 384)
            v = V[rows, :] + jnp.dot(R[...].astype(BF16), TI[c], preferred_element_type=F32)
            V[rows, :] = v
            if last:
                v = v.reshape(16, BAND, LON)
                PS[0] += jnp.sum(v, axis=0)
                PS[1] += jnp.sum(v * v, axis=0)
            return 0

        lax.fori_loop(0, SUBSTEPS, step, 0)

    def set_tables():
        for copy in small[1:]:
            copy.wait()
        row = lax.broadcasted_iota(jnp.int32, (256, LON), 0)
        for c in range(CHUNKS):
            t = TB[c].astype(F32)
            TF[c] = t.T.astype(BF16)
            twice = t * 2.0
            TI[c] = (jnp.where(row == 0, t, twice) if c == 0 else twice).astype(BF16)
        cl = CS[0]
        sl = CS[1]
        LF[0:LATS, 0:LATS] = cl
        LF[0:LATS, LATS:] = -sl
        LF[LATS:, 0:LATS] = sl
        LF[LATS:, LATS:] = cl
        LI[0:LATS, 0:LATS] = cl
        LI[0:LATS, LATS:] = sl
        LI[LATS:, 0:LATS] = -sl
        LI[LATS:, LATS:] = cl
        AW[...] = jnp.zeros((256, 256), F32)
        BT[...] = jnp.zeros((128, 128), F32)
        for l in range(2):
            for w_ref, a_ref in ((w1_ref, A1), (w2_ref, A2)):
                re = w_ref[l, 0].astype(F32)
                im = w_ref[l, 1].astype(F32)
                AW[0:96, 0:192] = jnp.concatenate([re, im], axis=1)
                AW[96:192, 0:192] = jnp.concatenate([-im, re], axis=1)
                a_ref[l] = AW[...].T[0:192, 0:192].astype(BF16)
            for part in range(2):
                BT[:, 0:96] = jnp.broadcast_to(b_ref[l, part : part + 1, :].astype(F32), (128, 96))
                B1[l, 96 * part : 96 * part + 96, :] = BT[...].T[0:96, :]

    def set_mean_inv(scale):
        for hb in range(3):
            for lb in range(6):
                t = hb * 6 + lb
                u = t + 18
                mean = AG[t // 5, t % 5] * scale * (1.0 / ALL_CH)
                spread = AG[u // 5, u % 5] * (scale * scale) * (1.0 / ALL_CH) - mean * mean
                MI[0, 8 * hb : 8 * hb + 8, 128 * lb : 128 * lb + 128] = mean
                MI[1, 8 * hb : 8 * hb + 8, 128 * lb : 128 * lb + 128] = lax.rsqrt(spread + norm_eps)

    by_energy = (0, AE, aes, aer)
    by_target = (1, AT, ats, atr)
    by_last = (0, AF, afs, afr)

    zero = jnp.zeros((BAND, LON), F32)
    for t in range(36, 40):
        ST[t] = jnp.zeros((8, 128), F32)

    def first_block(i, carry):
        x_copy(i).wait()

        def pair(j, carry):
            s1, s2 = carry
            rows = pl.ds(pl.multiple_of(i * 384 + j * 48, 48), 48)
            xx = X[rows, :].astype(F32)
            V[rows, :] = xx
            for t in range(2):
                v = xx[24 * t : 24 * t + 24]
                s1 = s1 + v
                s2 = s2 + v * v
            return s1, s2

        return lax.fori_loop(0, 8, pair, carry)

    s1, s2 = lax.fori_loop(0, 6, first_block, (zero, zero))
    PS[0] = s1
    PS[1] = s2
    small[0].wait()
    stats_out()
    pl.semaphore_wait(bar, len(ORDER) + len(CH_ORDER))
    rs_start()
    e_start()
    set_tables()
    rs_sum()
    ag_start()
    EX[1] = e_sum()
    ag_wait()
    rs_sent()
    ag_sent()
    e_sent()

    def layer(l, scale):
        set_mean_inv(scale)
        srow = scale[0:1, 0:1]
        forward_first(l, srow)
        forward_rest()

        def mid(c, _):
            middle_chunk(l, c)
            return 0

        lax.fori_loop(0, CHUNKS, mid, 0)

        def back(n, _):
            backward_unit(l, n // NSUB, n % NSUB, False)
            return 0

        lax.fori_loop(0, (CHUNKS - 1) * NSUB, back, 0)
        PS[...] = jnp.zeros((2, BAND, LON), F32)

        def back_last(u, _):
            backward_unit(l, CHUNKS - 1, u, True)
            return 0

        lax.fori_loop(0, NSUB, back_last, 0)
        stats_out()

        @pl.when(l == 0)
        def _():
            rs_start()
            e_start()
            row_start(*by_target)
            rs_sum()
            ag_start()
            EX[0] = e_sum()
            row_start(*by_energy)
            TC[...] = row_sum(*by_target)
            ag_wait()
            EN[...] = row_sum(*by_energy)
            rs_sent()
            ag_sent()
            row_sent(*by_target)
            row_sent(*by_energy)

        @pl.when(l == 1)
        def _():
            e_start()
            EX[0] = e_sum()
            row_start(*by_last)
            EN[...] = row_sum(*by_last)
            row_sent(*by_last)

        e_sent()

        def sent(n, _):
            c = n // NSUB
            u = n % NSUB
            unit_whole(SF, RF, fs, fr, c, u).wait_send()
            unit_whole(SB, RB, bs, br, c, u).wait_send()
            return 0

        lax.fori_loop(0, CHUNKS * NSUB, sent, 0)
        return jnp.sqrt(TC[...] / EN[...])

    scale = lax.fori_loop(0, 2, layer, jnp.ones((8, 128), F32))
    SC[...] = scale


def scale_kernel(v_ref, s_ref, o_hbm, out, so):
    def go(n):
        rows = slice(192 * n, 192 * n + 192)
        return pltpu.make_async_copy(out.at[rows], o_hbm.at[rows], so.at[n])

    scale = s_ref[0:1, 0:1]
    for n in range(12):
        rows = slice(192 * n, 192 * n + 192)
        out[rows, :] = (v_ref[rows, :] * scale).astype(BF16)
        go(n).start()
    for n in range(12):
        go(n).wait()


def per_device(field_in, ln_gain, ln_shift, mix_first, mix_bias, mix_second):
    vm = pl.BlockSpec(memory_space=pltpu.VMEM)
    hbm = pl.BlockSpec(memory_space=pl.ANY)
    dma = pltpu.SemaphoreType.DMA
    buf = pltpu.VMEM((CHUNKS, NSUB, N_LAT, SUBROWS, 128), BF16)
    unit = dma((CHUNKS, NSUB))
    summed, scale = pl.pallas_call(
        kernel,
        out_shape=(
            pltpu.VMEM((ROWS, LON), F32),
            pltpu.VMEM((8, 128), F32),
        ),
        in_specs=[hbm] * 9,
        out_specs=(vm, vm),
        scratch_shapes=[
            pltpu.VMEM((ROWS, LON), BF16),
            pltpu.VMEM((CHUNKS, 256, LON), BF16),
            pltpu.VMEM((2, LATS, LATS), BF16),
            pltpu.VMEM((2, 2, CHN, CHN), BF16),
            pltpu.VMEM((2, 2, CHN), BF16),
            pltpu.VMEM((2, 2, CHN, CHN), BF16),
            pltpu.VMEM((BAND, 128), F32),
            pltpu.SMEM((2, CHN), F32),
            pltpu.SMEM((2, CHN), F32),
            pltpu.VMEM((ROWS, LON), BF16),
            pltpu.VMEM((CHUNKS, LON, 256), BF16),
            pltpu.VMEM((CHUNKS, 256, LON), BF16),
            pltpu.VMEM((2 * LATS, 2 * LATS), BF16),
            pltpu.VMEM((2 * LATS, 2 * LATS), BF16),
            buf,
            buf,
            buf,
            buf,
            pltpu.VMEM((16, CHN, LATS), F32),
            pltpu.VMEM((384, 256), F32),
            pltpu.VMEM((384, 2 * LATS), BF16),
            pltpu.VMEM((384, 2 * LATS), BF16),
            pltpu.VMEM((256, 256), F32),
            pltpu.VMEM((2, 192, 192), BF16),
            pltpu.VMEM((2, 192, 192), BF16),
            pltpu.VMEM((128, 128), F32),
            pltpu.VMEM((2, 192, 128), F32),
            pltpu.VMEM((2, BAND, LON), F32),
            pltpu.VMEM((40, 8, 128), F32),
            pltpu.VMEM((8, 5, 8, 128), F32),
            pltpu.VMEM((5, 8, 128), F32),
            pltpu.VMEM((8, 5, 8, 128), F32),
            pltpu.VMEM((2, 1, 128), F32),
            pltpu.VMEM((8, 1, 128), F32),
            pltpu.VMEM((8, 1, 128), F32),
            pltpu.VMEM((8, 1, 128), F32),
            pltpu.VMEM((1, 128), F32),
            pltpu.VMEM((N_LAT, 1, 128), F32),
            pltpu.VMEM((8, 128), F32),
            pltpu.VMEM((8, 128), F32),
            pltpu.VMEM((2, BAND, LON), F32),
            dma((6,)),
            dma((8,)),
            unit,
            unit,
            unit,
            unit,
            dma((8,)),
            dma((8,)),
            dma((8,)),
            dma((8,)),
            dma((8,)),
            dma((8,)),
            dma((8,)),
            dma((8,)),
            dma((8,)),
            dma((8,)),
            dma((N_LAT,)),
            dma((N_LAT,)),
        ],
        compiler_params=pltpu.CompilerParams(
            collective_id=0, has_side_effects=True, vmem_limit_bytes=54 * 1024 * 1024
        ),
    )(
        field_in.reshape(ROWS, LON), lon_table(), lat_tables(), mix_first[:, :, 0], mix_bias[:, :, 0],
        mix_second[:, :, 0], area_table(), ln_gain, ln_shift,
    )
    out = pl.pallas_call(
        scale_kernel,
        out_shape=jax.ShapeDtypeStruct((ROWS, LON), BF16),
        in_specs=[vm, vm],
        out_specs=hbm,
        scratch_shapes=[pltpu.VMEM((ROWS, LON), BF16), dma((12,))],
        compiler_params=pltpu.CompilerParams(vmem_limit_bytes=8 * 1024 * 1024),
    )(
        pltpu.with_memory_space_constraint(summed, pltpu.VMEM),
        pltpu.with_memory_space_constraint(scale, pltpu.VMEM),
    )
    return out.reshape(CHN, BAND, LON)


def solution(mesh):
    finer = Mesh(mesh.devices.reshape(4, 4, 4, 2), ("lat_0", "lat_1", "ch_0", "ch_1"))
    in_specs = (
        P(CH, LAT, None),
        P(None, CH),
        P(None, CH),
        P(None, None, CH, None, None),
        P(None, None, CH, None),
        P(None, None, CH, None, None),
    )
    return jax.shard_map(
        per_device, mesh=finer, in_specs=in_specs, out_specs=P(CH, LAT, None), check_vma=False
    )
```

```python
import math

import jax
import jax.numpy as jnp
import numpy as np
from jax import lax
from jax.experimental import pallas as pl
from jax.experimental.pallas import tpu as pltpu
from jax.sharding import Mesh
from jax.sharding import PartitionSpec as P

CH = ("ch_0", "ch_1")
LAT = ("lat_0", "lat_1")
MESH = pl.DeviceIdType.MESH

norm_eps = 1e-05
shrink_level = 0.01

F32 = jnp.float32
BF16 = jnp.bfloat16

N_LAT = 16
BAND = 24
CHN = 96
ROWS = CHN * BAND
LON = 768
LATS = N_LAT * BAND
CHUNKS = 3
KL = 8
ALL_CH = 768
PIECE = 12 * BAND

ORDER = [
    (2, 2), (1, 2), (2, 1), (2, 3), (3, 2), (0, 2), (1, 1), (1, 3), (2, 0),
    (3, 1), (3, 3), (0, 1), (0, 3), (1, 0), (3, 0),
]
CH_ORDER = [(1, 0), (3, 0), (1, 1), (3, 1), (2, 0), (2, 1), (0, 1)]


NSUB = 6
SUBSTEPS = 6 // NSUB
SUBROWS = PIECE // NSUB


def trig(length, n, f):
    ang = (n * f % length) * (2.0 * math.pi / length)
    scale = 1.0 / math.sqrt(length)
    return np.cos(ang) * scale, np.sin(ang) * scale


def lon_table():
    row = np.arange(LON)
    kk = row // 8 % 16
    q = row // 128 % 2 * 8 + row % 8
    mode = q * BAND + row // 256 * KL + kk % KL
    cs, sn = trig(LON, mode[:, None], np.arange(LON)[None, :])
    return np.where((kk < KL)[:, None], cs, -sn).reshape(CHUNKS, 256, LON).astype(BF16)


def lat_tables():
    n = np.arange(LATS)
    cs, sn = trig(LATS, n[:, None], n[None, :])
    return np.stack([cs, sn]).astype(BF16)


def area_table():
    row = np.arange(LATS, dtype=np.float32).reshape(N_LAT, BAND, 1)
    area = np.cos((row + 0.5) * (math.pi / LATS) - 0.5 * math.pi)
    return np.broadcast_to(area, (N_LAT, BAND, 128)).astype(np.float32)


def kernel(
    x_hbm, tb_hbm, cs_hbm, w1_hbm, b_hbm, w2_hbm, area_hbm, gain_hbm, shift_hbm,
    V, SC,
    X, TB, CS, w1_ref, b_ref, w2_ref, area_ref, gain_ref, shift_ref, N, TF, TI, LF, LI, SF, RF, SB, RB, G, R, SP, MX, AW, A1, A2, BT, B1,
    PS, ST, RS, RED, AG, EX, AE, AT, AF, ES, EB, TC, EN, MI,
    xs, ts, fs, fr, bs, br, rss, rsr, ags, agr, aes, aer, ats, atr, afs, afr, es, er,
):
    y = lax.axis_index("lat_0")
    z = lax.axis_index("lat_1")
    cx = lax.axis_index("ch_0")
    ck = lax.axis_index("ch_1")
    me = y * 4 + z
    mc = cx * 2 + ck

    def x_copy(i):
        rows = pl.ds(pl.multiple_of(i * 192, 192), 192)
        return pltpu.make_async_copy(x_hbm.at[rows], X.at[rows], xs.at[i])

    for i in range(12):
        x_copy(i).start()
    small = [
        pltpu.make_async_copy(src, dst, ts.at[n])
        for n, (src, dst) in enumerate(
            (
                (area_hbm.at[me], area_ref),
                (tb_hbm, TB),
                (cs_hbm, CS),
                (w1_hbm, w1_ref),
                (b_hbm, b_ref),
                (w2_hbm, w2_ref),
                (gain_hbm, gain_ref),
                (shift_hbm, shift_ref),
            )
        )
    ]
    for copy in small:
        copy.start()

    def lat_to(a, b):
        yy = lax.rem(y + a, 4)
        zz = lax.rem(z + b, 4)
        return {"lat_0": yy, "lat_1": zz}, yy * 4 + zz

    def ch_to(a, b):
        xx = lax.rem(cx + a, 4)
        kk = lax.rem(ck + b, 2)
        return {"ch_0": xx, "ch_1": kk}, xx * 2 + kk

    bar = pltpu.get_barrier_semaphore()
    for a, b in ORDER:
        pl.semaphore_signal(bar, 1, device_id=lat_to(a, b)[0], device_id_type=MESH)
    for a, b in CH_ORDER:
        pl.semaphore_signal(bar, 1, device_id=ch_to(a, b)[0], device_id_type=MESH)

    def rcopy(src, dst, ss, rr, dev):
        return pltpu.make_async_remote_copy(
            src_ref=src, dst_ref=dst, send_sem=ss, recv_sem=rr, device_id=dev, device_id_type=MESH
        )

    def unit_start(sb, rb, ss, rr, c, u):
        for a, b in ORDER:
            dev, q = lat_to(a, b)
            rcopy(sb.at[c, u, q], rb.at[c, u, me], ss.at[c, u], rr.at[c, u], dev).start()
        rb[c, u, me] = sb[c, u, me]

    def unit_whole(sb, rb, ss, rr, c, u):
        peers = pl.ds(0, N_LAT - 1)
        dev = lat_to(1, 0)[0]
        return rcopy(sb.at[c, u, peers], rb.at[c, u, peers], ss.at[c, u], rr.at[c, u], dev)

    def stats_out():
        e = jnp.zeros((8, 128), F32)
        for hb in range(3):
            for lb in range(6):
                t = hb * 6 + lb
                rows, lanes = slice(8 * hb, 8 * hb + 8), slice(128 * lb, 128 * lb + 128)
                sq = PS[1, rows, lanes]
                ST[t] = PS[0, rows, lanes]
                ST[18 + t] = sq
                e = e + sq * area_ref[rows, :]
        ES[...] = jnp.sum(e, axis=0, keepdims=True)

    def e_copy(a, b):
        dev, q = lat_to(a, b)
        return rcopy(ES, EB.at[me], es.at[q], er.at[me], dev)

    def e_from(a, b):
        dev, p = lat_to(4 - a, 4 - b)
        return rcopy(ES, EB.at[p], es.at[p], er.at[p], dev)

    def rs_copy(a, b):
        dev, d = ch_to(a, b)
        return rcopy(ST.at[pl.ds(5 * d, 5)], RS.at[mc], rss.at[d], rsr.at[mc], dev)

    def rs_from(a, b):
        dev, d = ch_to(4 - a, 2 - b)
        return rcopy(ST.at[pl.ds(5 * d, 5)], RS.at[d], rss.at[d], rsr.at[d], dev)

    def ag_copy(a, b):
        dev, d = ch_to(a, b)
        return rcopy(RED, AG.at[mc], ags.at[d], agr.at[mc], dev)

    def ag_from(a, b):
        dev, d = ch_to(4 - a, 2 - b)
        return rcopy(RED, AG.at[d], ags.at[d], agr.at[d], dev)

    def rs_start():
        for a, b in CH_ORDER:
            rs_copy(a, b).start()
        RS[mc] = ST[pl.ds(5 * mc, 5)]

    def e_start():
        for a, b in ORDER:
            e_copy(a, b).start()
        EB[me] = ES[...]

    def rs_sum():
        for a, b in CH_ORDER:
            rs_from(a, b).wait_recv()
        tot = RS[0]
        for d in range(1, 8):
            tot = tot + RS[d]
        RED[...] = tot

    def e_sum():
        for a, b in ORDER:
            e_from(a, b).wait_recv()
        e = EB[0]
        for p in range(1, N_LAT):
            e = e + EB[p]
        return e

    def ag_start():
        for a, b in CH_ORDER:
            ag_copy(a, b).start()
        AG[mc] = RED[...]

    def ag_wait():
        for a, b in CH_ORDER:
            ag_from(a, b).wait_recv()

    def rs_sent():
        for a, b in CH_ORDER:
            rs_copy(a, b).wait_send()

    def ag_sent():
        for a, b in CH_ORDER:
            ag_copy(a, b).wait_send()

    def e_sent():
        for a, b in ORDER:
            e_copy(a, b).wait_send()

    def row_copy(n, dst, ss, rr, a, b):
        dev, d = ch_to(a, b)
        return rcopy(EX.at[n], dst.at[mc], ss.at[d], rr.at[mc], dev)

    def row_from(n, dst, ss, rr, a, b):
        dev, d = ch_to(4 - a, 2 - b)
        return rcopy(EX.at[n], dst.at[d], ss.at[d], rr.at[d], dev)

    def row_start(n, dst, ss, rr):
        for a, b in CH_ORDER:
            row_copy(n, dst, ss, rr, a, b).start()
        dst[mc] = EX[n]

    def row_sum(n, dst, ss, rr):
        for a, b in CH_ORDER:
            row_from(n, dst, ss, rr, a, b).wait_recv()
        return over_channels([dst[d] for d in range(8)])

    def row_sent(n, dst, ss, rr):
        for a, b in CH_ORDER:
            row_copy(n, dst, ss, rr, a, b).wait_send()

    def over_channels(tiles):
        e = tiles[0]
        for d in range(1, 8):
            e = e + tiles[d]
        e = jnp.sum(e, axis=1, keepdims=True)
        return jnp.broadcast_to(e, (8, 128))

    def lane_masks():
        lane = lax.broadcasted_iota(jnp.int32, (48, 128), 1) & 7
        return [lane == s for s in range(8)]

    def block_swap(parts, masks):
        rolled = [p if r == 0 else pltpu.roll(p, r, 1) for r, p in enumerate(parts)]
        out = []
        for q in range(8):
            acc = rolled[-q % 8]
            for s in range(1, 8):
                acc = jnp.where(masks[s], rolled[(s - q) % 8], acc)
            out.append(acc if q == 0 else pltpu.roll(acc, 128 - q, 1))
        return out

    def rows_of(ii):
        return pl.ds(pl.multiple_of(ii * 48, 48), 48)

    def forward_step(c, u, ii):
        base = pl.multiple_of((u * SUBSTEPS + ii) * 384, 384)
        R[...] = jnp.dot(N[pl.ds(base, 384), :], TF[c], preferred_element_type=F32)
        masks = lane_masks()
        for half in range(2):
            hs = slice(128 * half, 128 * half + 128)
            parts = [
                jnp.concatenate(
                    [R[24 * r : 24 * r + 24, hs], R[192 + 24 * r : 216 + 24 * r, hs]], axis=0
                )
                for r in range(8)
            ]
            for q, piece in enumerate(block_swap(parts, masks)):
                SF[c, u, 8 * half + q, rows_of(ii), :] = piece.astype(BF16)

    def normalize_step(l, srow, i, first):
        def pair(j, _):
            base = i * 384 + j * 48
            ch = i * 16 + j * 2
            for lb in range(2):
                ls = slice(384 * lb, 384 * lb + 384)
                mean = MI[0, :, ls]
                inv = MI[1, :, ls]
                both = []
                if first:
                    xx = X[pl.ds(pl.multiple_of(base, 48), 48), ls].astype(F32)
                for t in range(2):
                    rows = pl.ds(pl.multiple_of(base + 24 * t, 24), 24)
                    if first:
                        cur = xx[24 * t : 24 * t + 24]
                    else:
                        cur = (V[rows, ls] * srow).astype(BF16).astype(F32)
                    nrm = (cur - mean) * inv * gain_ref[l, ch + t] + shift_ref[l, ch + t]
                    nrm = nrm.astype(BF16).astype(F32)
                    V[rows, ls] = cur + nrm
                    both.append(nrm)
                N[pl.ds(pl.multiple_of(base, 48), 48), ls] = jnp.concatenate(both, axis=0).astype(BF16)
            return 0

        lax.fori_loop(0, 8, pair, 0)

    def forward_first(l, srow):
        def unit(u, _):
            def step(ii, _):
                @pl.when(l == 0)
                def _():
                    normalize_step(l, srow, u * SUBSTEPS + ii, True)

                @pl.when(l > 0)
                def _():
                    normalize_step(l, srow, u * SUBSTEPS + ii, False)

                forward_step(0, u, ii)
                return 0

            lax.fori_loop(0, SUBSTEPS, step, 0)
            unit_start(SF, RF, fs, fr, 0, u)
            return 0

        lax.fori_loop(0, NSUB, unit, 0)

    def forward_rest():
        def unit(n, _):
            c = n // NSUB
            u = n % NSUB

            def step(ii, _):
                forward_step(c, u, ii)
                return 0

            lax.fori_loop(0, SUBSTEPS, step, 0)
            unit_start(SF, RF, fs, fr, c, u)
            return 0

        lax.fori_loop(NSUB, CHUNKS * NSUB, unit, 0)

    def middle_chunk(l, c):
        def gather_unit(u, _):
            unit_whole(SF, RF, fs, fr, c, u).wait_recv()

            def gather(ii, _):
                i = u * SUBSTEPS + ii
                got = [RF[c, u, p, rows_of(ii), :].astype(F32) for p in range(N_LAT)]
                for j in range(2):
                    blk = jnp.concatenate([g[24 * j : 24 * j + 24] for g in got], axis=0)
                    t = blk.T.reshape(16, 8, LATS)
                    G[:, pl.ds(pl.multiple_of(i * 16 + 8 * j, 8), 8), :] = t
                return 0

            lax.fori_loop(0, SUBSTEPS, gather, 0)
            return 0

        lax.fori_loop(0, NSUB, gather_unit, 0)

        def mix(b, _):
            g_re = G[pl.ds(4 * b, 4)].reshape(384, LATS).astype(BF16)
            g_im = G[pl.ds(8 + 4 * b, 4)].reshape(384, LATS).astype(BF16)
            SP[...] = jnp.dot(
                jnp.concatenate([g_re, g_im], axis=1), LF[...], preferred_element_type=F32
            ).astype(BF16)
            bias = jnp.concatenate([B1[l]] * 3, axis=1)
            for k in range(4):
                rows = slice(96 * k, 96 * k + 96)
                both = jnp.concatenate([SP[rows, 0:LATS], SP[rows, LATS:]], axis=0)
                hid = jnp.dot(A1[l], both, preferred_element_type=F32) + bias
                hid = jnp.maximum(hid, 0.0).astype(BF16)
                m = jnp.dot(A2[l], hid, preferred_element_type=F32)
                m = (m - jnp.clip(m, -shrink_level, shrink_level)).astype(BF16)
                MX[rows, 0:LATS] = m[0:96]
                MX[rows, LATS:] = m[96:192]
            back = jnp.dot(MX[...], LI[...], preferred_element_type=F32)
            G[pl.ds(4 * b, 4)] = back[:, 0:LATS].reshape(4, CHN, LATS)
            G[pl.ds(8 + 4 * b, 4)] = back[:, LATS:].reshape(4, CHN, LATS)
            return 0

        lax.fori_loop(0, 2, mix, 0)

        def scatter_unit(u, _):
            def scatter(ii, _):
                i = u * SUBSTEPS + ii
                ts = []
                for j in range(2):
                    blk = G[:, pl.ds(pl.multiple_of(i * 16 + 8 * j, 8), 8), :].reshape(128, LATS)
                    ts.append(blk.T)
                for p in range(N_LAT):
                    piece = jnp.concatenate([t[24 * p : 24 * p + 24] for t in ts], axis=0)
                    SB[c, u, p, rows_of(ii), :] = piece.astype(BF16)
                return 0

            lax.fori_loop(0, SUBSTEPS, scatter, 0)
            unit_start(SB, RB, bs, br, c, u)
            return 0

        lax.fori_loop(0, NSUB, scatter_unit, 0)

    def backward_unit(l, c, u, last):
        unit_whole(SB, RB, bs, br, c, u).wait_recv()

        def step(ii, _):
            masks = lane_masks()
            for half in range(2):
                hs = slice(128 * half, 128 * half + 128)
                parts = [RB[c, u, 8 * half + q, rows_of(ii), :].astype(F32) for q in range(8)]
                for r, piece in enumerate(block_swap(parts, masks)):
                    R[24 * r : 24 * r + 24, hs] = piece[0:24]
                    R[192 + 24 * r : 216 + 24 * r, hs] = piece[24:48]
            rows = pl.ds(pl.multiple_of((u * SUBSTEPS + ii) * 384, 384), 384)
            v = V[rows, :] + jnp.dot(R[...].astype(BF16), TI[c], preferred_element_type=F32)
            V[rows, :] = v
            if last:
                v = v.reshape(16, BAND, LON)
                PS[0] += jnp.sum(v, axis=0)
                PS[1] += jnp.sum(v * v, axis=0)
            return 0

        lax.fori_loop(0, SUBSTEPS, step, 0)

    def set_tables():
        for copy in small[1:]:
            copy.wait()
        row = lax.broadcasted_iota(jnp.int32, (256, LON), 0)
        for c in range(CHUNKS):
            t = TB[c].astype(F32)
            TF[c] = t.T.astype(BF16)
            twice = t * 2.0
            TI[c] = (jnp.where(row == 0, t, twice) if c == 0 else twice).astype(BF16)
        cl = CS[0]
        sl = CS[1]
        LF[0:LATS, 0:LATS] = cl
        LF[0:LATS, LATS:] = -sl
        LF[LATS:, 0:LATS] = sl
        LF[LATS:, LATS:] = cl
        LI[0:LATS, 0:LATS] = cl
        LI[0:LATS, LATS:] = sl
        LI[LATS:, 0:LATS] = -sl
        LI[LATS:, LATS:] = cl
        AW[...] = jnp.zeros((256, 256), F32)
        BT[...] = jnp.zeros((128, 128), F32)
        for l in range(2):
            for w_ref, a_ref in ((w1_ref, A1), (w2_ref, A2)):
                re = w_ref[l, 0].astype(F32)
                im = w_ref[l, 1].astype(F32)
                AW[0:96, 0:192] = jnp.concatenate([re, im], axis=1)
                AW[96:192, 0:192] = jnp.concatenate([-im, re], axis=1)
                a_ref[l] = AW[...].T[0:192, 0:192].astype(BF16)
            for part in range(2):
                BT[:, 0:96] = jnp.broadcast_to(b_ref[l, part : part + 1, :].astype(F32), (128, 96))
                B1[l, 96 * part : 96 * part + 96, :] = BT[...].T[0:96, :]

    def set_mean_inv(scale):
        for hb in range(3):
            for lb in range(6):
                t = hb * 6 + lb
                u = t + 18
                mean = AG[t // 5, t % 5] * scale * (1.0 / ALL_CH)
                spread = AG[u // 5, u % 5] * (scale * scale) * (1.0 / ALL_CH) - mean * mean
                MI[0, 8 * hb : 8 * hb + 8, 128 * lb : 128 * lb + 128] = mean
                MI[1, 8 * hb : 8 * hb + 8, 128 * lb : 128 * lb + 128] = lax.rsqrt(spread + norm_eps)

    by_energy = (0, AE, aes, aer)
    by_target = (1, AT, ats, atr)
    by_last = (0, AF, afs, afr)

    zero = jnp.zeros((BAND, LON), F32)
    for t in range(36, 40):
        ST[t] = jnp.zeros((8, 128), F32)

    def first_block(i, carry):
        x_copy(i).wait()

        def pair(j, carry):
            s1, s2 = carry
            rows = pl.ds(pl.multiple_of(i * 192 + j * 48, 48), 48)
            xx = X[rows, :].astype(F32)
            for t in range(2):
                v = xx[24 * t : 24 * t + 24]
                s1 = s1 + v
                s2 = s2 + v * v
            return s1, s2

        return lax.fori_loop(0, 4, pair, carry)

    s1, s2 = lax.fori_loop(0, 12, first_block, (zero, zero))
    PS[0] = s1
    PS[1] = s2
    small[0].wait()
    stats_out()
    pl.semaphore_wait(bar, len(ORDER) + len(CH_ORDER))
    rs_start()
    set_tables()
    rs_sum()
    ag_start()
    e_start()
    ag_wait()
    rs_sent()
    ag_sent()

    def layer(l, scale):
        set_mean_inv(scale)
        srow = scale[0:1, 0:1]
        forward_first(l, srow)
        forward_rest()

        @pl.when(l == 0)
        def _():
            EX[1] = e_sum()
            e_sent()
            row_start(*by_target)

        def mid(c, _):
            middle_chunk(l, c)
            return 0

        lax.fori_loop(0, CHUNKS, mid, 0)

        def back(n, _):
            backward_unit(l, n // NSUB, n % NSUB, False)
            return 0

        lax.fori_loop(0, (CHUNKS - 1) * NSUB, back, 0)
        PS[...] = jnp.zeros((2, BAND, LON), F32)

        def back_last(u, _):
            backward_unit(l, CHUNKS - 1, u, True)
            return 0

        lax.fori_loop(0, NSUB, back_last, 0)
        stats_out()

        @pl.when(l == 0)
        def _():
            rs_start()
            e_start()
            rs_sum()
            ag_start()
            EX[0] = e_sum()
            row_start(*by_energy)
            TC[...] = row_sum(*by_target)
            ag_wait()
            EN[...] = row_sum(*by_energy)
            rs_sent()
            ag_sent()
            row_sent(*by_target)
            row_sent(*by_energy)

        @pl.when(l == 1)
        def _():
            e_start()
            EX[0] = e_sum()
            row_start(*by_last)
            EN[...] = row_sum(*by_last)
            row_sent(*by_last)

        e_sent()

        def sent(n, _):
            c = n // NSUB
            u = n % NSUB
            unit_whole(SF, RF, fs, fr, c, u).wait_send()
            unit_whole(SB, RB, bs, br, c, u).wait_send()
            return 0

        lax.fori_loop(0, CHUNKS * NSUB, sent, 0)
        return jnp.sqrt(TC[...] / EN[...])

    scale = lax.fori_loop(0, 2, layer, jnp.ones((8, 128), F32))
    SC[...] = scale


def scale_kernel(v_ref, s_ref, o_hbm, out, so):
    def go(n):
        rows = slice(96 * n, 96 * n + 96)
        return pltpu.make_async_copy(out.at[rows], o_hbm.at[rows], so.at[n])

    scale = s_ref[0:1, 0:1]
    for n in range(24):
        rows = slice(96 * n, 96 * n + 96)
        out[rows, :] = (v_ref[rows, :] * scale).astype(BF16)
        go(n).start()
    for n in range(24):
        go(n).wait()


def per_device(field_in, ln_gain, ln_shift, mix_first, mix_bias, mix_second):
    vm = pl.BlockSpec(memory_space=pltpu.VMEM)
    hbm = pl.BlockSpec(memory_space=pl.ANY)
    dma = pltpu.SemaphoreType.DMA
    buf = pltpu.VMEM((CHUNKS, NSUB, N_LAT, SUBROWS, 128), BF16)
    unit = dma((CHUNKS, NSUB))
    summed, scale = pl.pallas_call(
        kernel,
        out_shape=(
            pltpu.VMEM((ROWS, LON), F32),
            pltpu.VMEM((8, 128), F32),
        ),
        in_specs=[hbm] * 9,
        out_specs=(vm, vm),
        scratch_shapes=[
            pltpu.VMEM((ROWS, LON), BF16),
            pltpu.VMEM((CHUNKS, 256, LON), BF16),
            pltpu.VMEM((2, LATS, LATS), BF16),
            pltpu.VMEM((2, 2, CHN, CHN), BF16),
            pltpu.VMEM((2, 2, CHN), BF16),
            pltpu.VMEM((2, 2, CHN, CHN), BF16),
            pltpu.VMEM((BAND, 128), F32),
            pltpu.SMEM((2, CHN), F32),
            pltpu.SMEM((2, CHN), F32),
            pltpu.VMEM((ROWS, LON), BF16),
            pltpu.VMEM((CHUNKS, LON, 256), BF16),
            pltpu.VMEM((CHUNKS, 256, LON), BF16),
            pltpu.VMEM((2 * LATS, 2 * LATS), BF16),
            pltpu.VMEM((2 * LATS, 2 * LATS), BF16),
            buf,
            buf,
            buf,
            buf,
            pltpu.VMEM((16, CHN, LATS), F32),
            pltpu.VMEM((384, 256), F32),
            pltpu.VMEM((384, 2 * LATS), BF16),
            pltpu.VMEM((384, 2 * LATS), BF16),
            pltpu.VMEM((256, 256), F32),
            pltpu.VMEM((2, 192, 192), BF16),
            pltpu.VMEM((2, 192, 192), BF16),
            pltpu.VMEM((128, 128), F32),
            pltpu.VMEM((2, 192, 128), F32),
            pltpu.VMEM((2, BAND, LON), F32),
            pltpu.VMEM((40, 8, 128), F32),
            pltpu.VMEM((8, 5, 8, 128), F32),
            pltpu.VMEM((5, 8, 128), F32),
            pltpu.VMEM((8, 5, 8, 128), F32),
            pltpu.VMEM((2, 1, 128), F32),
            pltpu.VMEM((8, 1, 128), F32),
            pltpu.VMEM((8, 1, 128), F32),
            pltpu.VMEM((8, 1, 128), F32),
            pltpu.VMEM((1, 128), F32),
            pltpu.VMEM((N_LAT, 1, 128), F32),
            pltpu.VMEM((8, 128), F32),
            pltpu.VMEM((8, 128), F32),
            pltpu.VMEM((2, BAND, LON), F32),
            dma((12,)),
            dma((8,)),
            unit,
            unit,
            unit,
            unit,
            dma((8,)),
            dma((8,)),
            dma((8,)),
            dma((8,)),
            dma((8,)),
            dma((8,)),
            dma((8,)),
            dma((8,)),
            dma((8,)),
            dma((8,)),
            dma((N_LAT,)),
            dma((N_LAT,)),
        ],
        compiler_params=pltpu.CompilerParams(
            collective_id=0, has_side_effects=True, vmem_limit_bytes=54 * 1024 * 1024
        ),
    )(
        field_in.reshape(ROWS, LON), lon_table(), lat_tables(), mix_first[:, :, 0], mix_bias[:, :, 0],
        mix_second[:, :, 0], area_table(), ln_gain, ln_shift,
    )
    out = pl.pallas_call(
        scale_kernel,
        out_shape=jax.ShapeDtypeStruct((ROWS, LON), BF16),
        in_specs=[vm, vm],
        out_specs=hbm,
        scratch_shapes=[pltpu.VMEM((ROWS, LON), BF16), dma((24,))],
        compiler_params=pltpu.CompilerParams(vmem_limit_bytes=8 * 1024 * 1024),
    )(
        pltpu.with_memory_space_constraint(summed, pltpu.VMEM),
        pltpu.with_memory_space_constraint(scale, pltpu.VMEM),
    )
    return out.reshape(CHN, BAND, LON)


def solution(mesh):
    finer = Mesh(mesh.devices.reshape(4, 4, 4, 2), ("lat_0", "lat_1", "ch_0", "ch_1"))
    in_specs = (
        P(CH, LAT, None),
        P(None, CH),
        P(None, CH),
        P(None, None, CH, None, None),
        P(None, None, CH, None),
        P(None, None, CH, None, None),
    )
    return jax.shard_map(
        per_device, mesh=finer, in_specs=in_specs, out_specs=P(CH, LAT, None), check_vma=False
    )
```
